8 devices in a mesh: dp: 1 (over z), ep: 2 (over y), tp: 4 (over x, core).
Axes of the slice: x: 2, y: 2, z: 1, core: 2. Of those that a mesh axis runs over, the one named last changes fastest.
Arguments:
- tokens: bfloat16 [8192, 768], P(('dp', 'ep', 'tp'))
- expert_ids: int32 [8192, 4], P(('dp', 'ep', 'tp'))
- gates: float32 [8192, 4], P(('dp', 'ep', 'tp'))
- w_gate: bfloat16 [16, 768, 10752], P('ep', None, 'tp')
- w_up: bfloat16 [16, 768, 10752], P('ep', None, 'tp')
- w_down: bfloat16 [16, 10752, 768], P('ep', 'tp')
Outputs:
- output: bfloat16 [8192, 768], P(('dp', 'ep', 'tp'))
All inputs are finite; a program needn't handle non-finite values.
Results may differ from the reference program's by a relative error of at most 0.00998244.
Values are sent between devices in bfloat16 or wider.
A program may use at most 1 GiB of HBM per device.

```python
import jax
import jax.numpy as jnp
from jax import lax

D_MODEL = 768
FF_DIM = 10752
EXPERTS = 16
TOP_K = 4
TOK_DEV = 1024
SOURCES = 8

CAPACITY = 5 * TOP_K * TOK_DEV // (4 * EXPERTS)
TOK_PART = SOURCES * TOK_DEV


def draw_routes(dev_key):
    key_perm, key_rot, key_lab = jax.random.split(dev_key, 3)
    fair_share = TOP_K * TOK_DEV // EXPERTS
    row_order = jax.random.permutation(key_perm, TOK_DEV)
    rotate = jax.random.randint(key_rot, (TOK_DEV, 1), 0, TOP_K)
    col_pos = (jnp.arange(TOP_K)[None, :] + rotate) % TOP_K
    labels = (row_order[:, None] * TOP_K + col_pos) % EXPERTS
    free_rows = jnp.logical_not(jnp.any(labels == 0, axis=1)).astype(jnp.int32)
    chosen = jnp.logical_and(free_rows > 0, jnp.cumsum(free_rows) <= fair_share // 2)
    first_col = (jnp.arange(TOP_K) == 0)[None, :]
    labels = jnp.where(jnp.logical_and(chosen[:, None], first_col), 0, labels)
    relabel = jax.random.permutation(key_lab, EXPERTS)
    return relabel[labels].astype(jnp.int32)


def setup_inputs(seed: int = 0, part: int = 0) -> dict:
    part_key = jax.random.fold_in(jax.random.key(seed), part)
    key_x, key_idx, key_gate = jax.random.split(part_key, 3)
    key_w1, key_w3, key_w2 = jax.random.split(jax.random.key(seed + 1), 3)
    tokens = jax.random.normal(key_x, (TOK_PART, D_MODEL), jnp.float32).astype(jnp.bfloat16)
    expert_ids = jax.vmap(draw_routes)(jax.random.split(key_idx, SOURCES)).reshape(TOK_PART, TOP_K)
    gates = jax.random.uniform(key_gate, (TOK_PART, TOP_K), jnp.float32, 0.5, 1.5) * TOP_K ** -0.5
    w_gate = (jax.random.normal(key_w1, (EXPERTS, D_MODEL, FF_DIM), jnp.float32) * D_MODEL ** -0.5).astype(jnp.bfloat16)
    w_up = (jax.random.normal(key_w3, (EXPERTS, D_MODEL, FF_DIM), jnp.float32) * D_MODEL ** -0.5).astype(jnp.bfloat16)
    w_down = (jax.random.normal(key_w2, (EXPERTS, FF_DIM, D_MODEL), jnp.float32) * FF_DIM ** -0.5).astype(jnp.bfloat16)
    return {"tokens": tokens, "expert_ids": expert_ids, "gates": gates, "w_gate": w_gate, "w_up": w_up, "w_down": w_down}


def slot_numbers(routes):
    hit_count = jnp.sum((routes[:, :, None] == jnp.arange(EXPERTS)).astype(jnp.int32), axis=1)
    before = jnp.cumsum(hit_count, axis=0) - hit_count
    return jnp.take_along_axis(before, routes, axis=1)


def dispatch_rows(dev_rows, dest_slot):
    row_ids = jnp.broadcast_to(jnp.arange(TOK_DEV, dtype=jnp.int32)[:, None], dest_slot.shape)
    owner_row = jnp.full((EXPERTS * CAPACITY,), TOK_DEV, jnp.int32).at[dest_slot.reshape(-1)].set(row_ids.reshape(-1), mode="drop")
    return jnp.take(dev_rows, owner_row, axis=0, mode="fill", fill_value=0).reshape(EXPERTS, CAPACITY, D_MODEL)


def expert_ffn(blk_rows, gate_mat, up_mat, down_mat):
    act_gate = jnp.dot(blk_rows, gate_mat, preferred_element_type=jnp.float32)
    act_up = jnp.dot(blk_rows, up_mat, preferred_element_type=jnp.float32)
    hidden = (jax.nn.silu(act_gate) * act_up).astype(jnp.bfloat16)
    return jnp.dot(hidden, down_mat, preferred_element_type=jnp.float32).astype(jnp.bfloat16)


def reference(tokens, expert_ids, gates, w_gate, w_up, w_down):
    dev_rows = tokens.reshape(SOURCES, TOK_DEV, D_MODEL)
    routes = expert_ids.reshape(SOURCES, TOK_DEV, TOP_K)
    dev_gates = gates.reshape(SOURCES, TOK_DEV, TOP_K)
    slot_ids = jax.vmap(slot_numbers)(routes)
    kept_mask = slot_ids < CAPACITY
    dest_slot = jnp.where(kept_mask, routes * CAPACITY + slot_ids, EXPERTS * CAPACITY)
    buffers = jax.vmap(dispatch_rows)(dev_rows, dest_slot)

    def per_expert(operands):
        blocks, gate_mat, up_mat, down_mat = operands
        return lax.map(lambda one_block: expert_ffn(one_block, gate_mat, up_mat, down_mat), blocks)

    results = lax.map(per_expert, (jnp.swapaxes(buffers, 0, 1), w_gate, w_up, w_down))
    out_table = jnp.swapaxes(results, 0, 1).reshape(SOURCES, EXPERTS * CAPACITY, D_MODEL)
    picked = jax.vmap(lambda src_table, src_dest: jnp.take(src_table, src_dest, axis=0, mode="fill", fill_value=0))(out_table, dest_slot)
    gate_kept = jnp.where(kept_mask, dev_gates, 0.0)
    mixed_rows = jnp.sum(gate_kept[..., None] * picked.astype(jnp.float32), axis=2)
    return mixed_rows.astype(jnp.bfloat16).reshape(TOK_PART, D_MODEL)
```

```python
import functools
import jax
import jax.numpy as jnp
from jax import lax
from jax.experimental import pallas as pl
from jax.experimental.pallas import tpu as pltpu

from jax.sharding import PartitionSpec as P


def add_pair(a, b):
    return (a.astype(jnp.float32) + b.astype(jnp.float32)).astype(jnp.bfloat16)

CHUNK = 512

def chunks_of(width, step):
    return [(lo, min(step, width - lo)) for lo in range(0, width, step)]

def phase_kernel(cap, small, sources, pieces, waits, *refs):
    route_refs, refs = refs[:sources], refs[sources:]
    tok_hbm, refs = refs[:pieces], refs[pieces:]
    wg_hbm, wu_hbm, wd_hbm = refs[:3]
    refs = refs[3 + waits:]
    out_hbm = refs[:sources]
    (wg_buf, wu_buf, wd_buf, tok_ref, acc_ref, out_buf, slot_lane, gate_lane, slot_sub, h_ref, count_ref, sems, tok_sems) = refs[sources:]
    _, toks, d_model = tok_ref.shape
    top_k = route_refs[0].shape[0] // 2
    experts, _, ff = wg_hbm.shape
    blocks = toks // 128

    def weight_copies(e, buf):
        return [
            pltpu.make_async_copy(wg_hbm.at[e], wg_buf.at[buf], sems.at[buf, 0]),
            pltpu.make_async_copy(wu_hbm.at[e], wu_buf.at[buf], sems.at[buf, 1]),
            pltpu.make_async_copy(wd_hbm.at[e], wd_buf.at[buf], sems.at[buf, 2]),
        ]

    size = sources * toks // pieces
    tok_copies = [
        pltpu.make_async_copy(tok_hbm[p], tok_ref.at[p * size // toks, pl.ds(p * size % toks, size), :], tok_sems.at[p])
        for p in range(pieces)
    ]
    for copy in tok_copies + weight_copies(0, 0):
        copy.start()

    tri = (lax.broadcasted_iota(jnp.int32, (128, 128), 0) < lax.broadcasted_iota(jnp.int32, (128, 128), 1)).astype(jnp.bfloat16)
    expert_row = lax.broadcasted_iota(jnp.int32, (experts, toks), 0).astype(jnp.float32)
    for s in range(sources):
        hit = jnp.zeros((experts, toks), jnp.float32)
        gate = jnp.zeros((experts, toks), jnp.float32)
        for j in range(top_k):
            same = route_refs[s][j:j + 1, :] == expert_row
            hit = jnp.where(same, 1.0, hit)
            gate = jnp.where(same, route_refs[s][top_k + j:top_k + j + 1, :], gate)
        stacked = jnp.concatenate([hit[:, b * 128:(b + 1) * 128] for b in range(blocks)], axis=0)
        inner = jnp.dot(stacked.astype(jnp.bfloat16), tri, preferred_element_type=jnp.float32)
        base = jnp.zeros((experts, 1), jnp.float32)
        pieces = []
        for b in range(blocks):
            part = inner[b * experts:(b + 1) * experts, :]
            pieces.append(part + base)
            base = base + part[:, 127:128] + hit[:, b * 128 + 127:b * 128 + 128]
        slot = jnp.concatenate(pieces, axis=1)
        slot = jnp.where((hit > 0) & (slot < cap), slot, -1.0)
        slot_lane[s] = slot
        gate_lane[s] = gate
        slot_sub[s] = jnp.transpose(slot)
        for e in range(experts):
            count_ref[s, e] = jnp.minimum(jnp.max(slot[e:e + 1, :]), cap - 1.0).astype(jnp.int32) + 1
    acc_ref[...] = jnp.zeros_like(acc_ref)
    for copy in tok_copies:
        copy.wait()

    def tile(e, s, buf, rows):
        slot_row = slot_lane[s, pl.ds(e, 1), :]
        pick = lax.broadcasted_iota(jnp.int32, (rows, toks), 0).astype(jnp.float32) == slot_row
        row_gate = jnp.sum(jnp.where(pick, gate_lane[s, pl.ds(e, 1), :], 0.0), axis=1, keepdims=True)
        x = jnp.dot(pick.astype(jnp.bfloat16), tok_ref[s], preferred_element_type=jnp.float32).astype(jnp.bfloat16)
        for lo, width in chunks_of(ff, CHUNK):
            a = jnp.dot(x, wg_buf[buf, :, lo:lo + width], preferred_element_type=jnp.float32)
            b = jnp.dot(x, wu_buf[buf, :, lo:lo + width], preferred_element_type=jnp.float32)
            h_ref[:rows, lo:lo + width] = (a * jax.nn.sigmoid(a) * b).astype(jnp.bfloat16)
        y = jnp.dot(h_ref[:rows, :], wd_buf[buf], preferred_element_type=jnp.float32)
        y = (y * row_gate).astype(jnp.bfloat16)
        col = slot_sub[s]
        mine = lax.broadcasted_iota(jnp.int32, col.shape, 1) == e
        slot_col = jnp.sum(jnp.where(mine, col, 0.0), axis=1, keepdims=True)
        put = (slot_col == lax.broadcasted_iota(jnp.int32, (toks, rows), 1).astype(jnp.float32)).astype(jnp.bfloat16)
        acc_ref[s] += jnp.dot(put, y, preferred_element_type=jnp.float32)

    def expert_step(e, _):
        buf = lax.rem(e, 2)
        for copy in weight_copies(e, buf):
            copy.wait()

        @pl.when(e + 1 < experts)
        def _():
            for copy in weight_copies(e + 1, 1 - buf):
                copy.start()

        def source_step(s, _):
            n = count_ref[s, e]

            @pl.when((n > 0) & (n <= small))
            def _():
                tile(e, s, buf, small)

            @pl.when(n > small)
            def _():
                tile(e, s, buf, cap)
            return 0

        lax.fori_loop(0, sources, source_step, 0)
        return 0

    lax.fori_loop(0, experts, expert_step, 0)
    for s in range(sources):
        out_buf[s] = acc_ref[s].astype(out_buf.dtype)
    out_copies = [pltpu.make_async_copy(out_buf.at[s], out_hbm[s], tok_sems.at[s]) for s in range(sources)]
    for copy in out_copies:
        copy.start()
    for copy in out_copies:
        copy.wait()


def phase(routes, toks, wg, wu, wd, cap, after=()):
    sources = len(routes)
    tok_dev, d_model = routes[0].shape[1], toks[0].shape[1]
    experts, _, ff = wg.shape
    small = min(cap, 256)
    vm = pl.BlockSpec(memory_space=pltpu.VMEM)
    hbm = pl.BlockSpec(memory_space=pl.ANY)
    return pl.pallas_call(
        functools.partial(phase_kernel, cap, small, sources, len(toks), len(after)),
        out_shape=[jax.ShapeDtypeStruct((tok_dev, d_model), jnp.bfloat16)] * sources,
        in_specs=[vm] * sources + [hbm] * (len(toks) + 3 + len(after)),
        out_specs=[hbm] * sources,
        scratch_shapes=[
            pltpu.VMEM((2, d_model, ff), jnp.bfloat16),
            pltpu.VMEM((2, d_model, ff), jnp.bfloat16),
            pltpu.VMEM((2, ff, d_model), jnp.bfloat16),
            pltpu.VMEM((sources, tok_dev, d_model), jnp.bfloat16),
            pltpu.VMEM((sources, tok_dev, d_model), jnp.float32),
            pltpu.VMEM((sources, tok_dev, d_model), jnp.bfloat16),
            pltpu.VMEM((sources, experts, tok_dev), jnp.float32),
            pltpu.VMEM((sources, experts, tok_dev), jnp.float32),
            pltpu.VMEM((sources, tok_dev, experts), jnp.float32),
            pltpu.VMEM((cap, ff), jnp.bfloat16),
            pltpu.SMEM((sources, experts), jnp.int32),
            pltpu.SemaphoreType.DMA((2, 3)),
            pltpu.SemaphoreType.DMA((len(toks),)),
        ],
        compiler_params=pltpu.CompilerParams(vmem_limit_bytes=60 * 2**20),
        cost_estimate=pl.CostEstimate(
            flops=6 * sources * experts * small * d_model * ff,
            bytes_accessed=6 * experts * d_model * ff,
            transcendentals=0,
        ),
        name="moe_phase",
    )(*routes, *toks, wg, wu, wd, *after)


def solution(mesh):
    ep_size = mesh.shape["ep"]
    tp_size = mesh.shape["tp"]
    row_spec = P(("dp", "ep", "tp"), None)
    axes = ("dp", "ep", "tp")
    ranks = [(d, y, t) for d in range(mesh.shape["dp"]) for y in range(ep_size) for t in range(tp_size)]

    def rank_of(d, y, t):
        return (d * ep_size + y) * tp_size + t

    def shift(arr, flip_ep, flip_tp):
        return lax.ppermute(arr, axes, [(rank_of(*r), rank_of(r[0], r[1] ^ flip_ep, r[2] ^ flip_tp)) for r in ranks])

    def local_layer(tokens, expert_ids, gates, w_gate, w_up, w_down):
        tok_dev, d_model = tokens.shape
        top_k = expert_ids.shape[1]
        local_experts = w_gate.shape[0]
        capacity = 5 * top_k * tok_dev // (4 * local_experts * ep_size)
        first = (lax.axis_index("ep") * local_experts).astype(jnp.float32)
        routes = jnp.concatenate([expert_ids.T.astype(jnp.float32), gates.T], axis=0)

        def run(tok_list, route_list, *after):
            return phase([r.at[:top_k].add(-first) for r in route_list], tok_list, w_gate, w_up, w_down, capacity, after)

        half = tok_dev // 2
        r_x, r_y = shift(routes, 0, 2), shift(routes, 1, 0)
        t_x, t_y = shift(tokens, 0, 2), shift(tokens, 1, 0)
        r_p, r_xp, r_yp = shift(routes, 0, 1), shift(routes, 0, 3), shift(routes, 1, 1)
        r_d, r_dp = shift(routes, 1, 2), shift(routes, 1, 3)
        t_p = shift(tokens, 0, 1)
        t_xp, t_yp = shift(t_x, 0, 1), shift(t_y, 0, 1)
        halves = [shift(t_x[:half], 1, 0), shift(t_y[half:], 0, 2)]

        (own,) = run([tokens], [routes])
        x_a, x_b = run([t_x, t_xp], [r_x, r_xp], own)
        x_in = shift(x_b, 0, 1)
        d_lo, d_hi, _ = lax.optimization_barrier((*halves, x_a))
        d_toks = [d_lo, d_hi, shift(d_lo, 0, 1), shift(d_hi, 0, 1)]
        y_a, y_b = run([t_y, t_yp], [r_y, r_yp], x_a)
        x_sum = add_pair(x_a, x_in)
        x_back = shift(x_sum, 0, 2)
        y_in = shift(y_b, 0, 1)
        d_a, d_b = run(d_toks, [r_d, r_dp], x_sum, y_a)
        y_sum = add_pair(y_a, y_in)
        y_back = shift(y_sum, 1, 0)
        d_in = shift(d_b, 0, 1)
        d_sum = add_pair(d_a, d_in)
        d_back = shift(d_sum, 1, 2)
        (part,) = run([t_p], [r_p], y_sum, d_sum)
        p_back = shift(part, 0, 1)
        total = own.astype(jnp.float32)
        for piece in (p_back, x_back, y_back, d_back):
            total += piece.astype(jnp.float32)
        return total.astype(jnp.bfloat16)

    return jax.shard_map(
        local_layer,
        mesh=mesh,
        in_specs=(row_spec, row_spec, row_spec, P("ep", None, "tp"), P("ep", None, "tp"), P("ep", "tp", None)),
        out_specs=row_spec,
        check_vma=False,
    )
```

```python
import functools
import jax
import jax.numpy as jnp
from jax import lax
from jax.experimental import pallas as pl
from jax.experimental.pallas import tpu as pltpu

from jax.sharding import PartitionSpec as P


def add_pair(a, b):
    return (a.astype(jnp.float32) + b.astype(jnp.float32)).astype(jnp.bfloat16)


CHUNK = 512
BLOCK = 256
PARTS = 3
WINDOW = 128


def chunks_of(width, step):
    return [(lo, min(step, width - lo)) for lo in range(0, width, step)]


def phase_kernel(cap, small, pieces, waits, route_ref, *refs):
    tok_hbm, refs = refs[:pieces], refs[pieces:]
    wg_hbm, wu_hbm, wd_hbm = refs[:3]
    refs = refs[3 + waits:]
    sources, lines, toks = route_ref.shape
    out_hbm = refs[:sources]
    (wg_buf, wu_buf, wd_buf, tok_ref, rows_ref, pick_ref, yblk_ref, acc_ref, slot_lane, gate_lane, slot_sub, row_gate, h_ref,
     base_ref, sems, tok_sems, out_sem) = refs[sources:]
    top_k = lines // 2
    experts, _, ff = wg_hbm.shape
    blocks = toks // BLOCK
    stride = cap + WINDOW

    def weight_copies(e, buf):
        copies = []
        for i, (src, dst) in enumerate(((wg_hbm, wg_buf), (wu_hbm, wu_buf), (wd_hbm, wd_buf))):
            rows = src.shape[1] // PARTS
            for p in range(PARTS):
                part = pl.ds(p * rows, rows)
                copies.append(pltpu.make_async_copy(src.at[e, part, :], dst.at[buf, part, :], sems.at[buf, i * PARTS + p]))
        return copies

    size = sources * toks // pieces
    tok_copies = [
        pltpu.make_async_copy(tok_hbm[p], tok_ref.at[p * size // toks, pl.ds(p * size % toks, size), :], tok_sems.at[p])
        for p in range(pieces)
    ]
    for copy in tok_copies:
        copy.start()

    tri = (lax.broadcasted_iota(jnp.int32, (128, 128), 0) < lax.broadcasted_iota(jnp.int32, (128, 128), 1)).astype(jnp.bfloat16)
    expert_row = lax.broadcasted_iota(jnp.int32, (experts, toks), 0).astype(jnp.float32)

    def number(s, _):
        hit = jnp.zeros((experts, toks), jnp.float32)
        gate = jnp.zeros((experts, toks), jnp.float32)
        for j in range(top_k):
            same = route_ref[s, j:j + 1, :] == expert_row
            hit = jnp.where(same, 1.0, hit)
            gate = jnp.where(same, route_ref[s, top_k + j:top_k + j + 1, :], gate)
        lanes = [hit[:, lo:lo + 128] for lo in range(0, toks, 128)]
        inner = jnp.dot(jnp.concatenate(lanes, axis=0).astype(jnp.bfloat16), tri, preferred_element_type=jnp.float32)
        base = jnp.zeros((experts, 1), jnp.float32)
        parts = []
        for i in range(len(lanes)):
            if i * 128 % BLOCK == 0:
                for e in range(experts):
                    base_ref[s, i * 128 // BLOCK, e] = base[e, 0].astype(jnp.int32)
            part = inner[i * experts:(i + 1) * experts, :]
            parts.append(part + base)
            base = base + part[:, 127:128] + lanes[i][:, 127:128]
        for e in range(experts):
            base_ref[s, blocks, e] = base[e, 0].astype(jnp.int32)
        slot = jnp.concatenate(parts, axis=1)
        slot = jnp.where((hit > 0) & (slot < cap), slot, -1.0)
        slot_lane[s] = slot
        gate_lane[s] = gate
        slot_sub[s] = jnp.transpose(slot)
        return 0

    lax.fori_loop(0, sources, number, 0)
    rows_ref[...] = jnp.zeros_like(rows_ref)
    row_gate[...] = jnp.zeros_like(row_gate)
    for copy in tok_copies:
        copy.wait()
    for copy in weight_copies(0, 0):
        copy.start()

    def bounds(s, b, e):
        begin = jnp.minimum(base_ref[s, b, e], cap)
        end = jnp.minimum(base_ref[s, b + 1, e], cap)
        return begin, end, (begin // 16) * 16

    def extra_windows(s, b):
        most = jnp.int32(0)
        for e in range(experts):
            _, end, at = bounds(s, b, e)
            most = jnp.maximum(most, end - at)
        return jnp.maximum(most - 1, 0) // WINDOW

    def put_rows(s, e, at, begin, new, gates):
        head = pl.ds(pl.multiple_of(e * stride + at, 16), 16)
        rest = pl.ds(pl.multiple_of(e * stride + at + 16, 16), WINDOW - 16)
        old = lax.broadcasted_iota(jnp.int32, (16, 1), 0) + at < begin
        rows_ref[s, head, :] = jnp.where(old, rows_ref[s, head, :].astype(jnp.float32), new[:16]).astype(jnp.bfloat16)
        row_gate[s, head, :] = jnp.where(old, row_gate[s, head, :], gates[:16])
        rows_ref[s, rest, :] = new[16:].astype(jnp.bfloat16)
        row_gate[s, rest, :] = gates[16:]

    def dispatch(i, _):
        s, b = i // blocks, lax.rem(i, blocks)
        span = pl.ds(pl.multiple_of(b * BLOCK, BLOCK), BLOCK)
        local = lax.broadcasted_iota(jnp.int32, (WINDOW, BLOCK), 0)

        def one_hot(e, at):
            return (local + at).astype(jnp.float32) == slot_lane[s, e:e + 1, span]

        def gates_of(pick, e):
            return jnp.sum(jnp.where(pick, gate_lane[s, e:e + 1, span], 0.0), axis=1, keepdims=True)

        gates = []
        for e in range(experts):
            _, _, at = bounds(s, b, e)
            pick = one_hot(e, at)
            gates.append(gates_of(pick, e))
            pick_ref[e * WINDOW:(e + 1) * WINDOW, :] = pick.astype(jnp.bfloat16)
        new = jnp.dot(pick_ref[...], tok_ref[s, span, :], preferred_element_type=jnp.float32)
        for e in range(experts):
            begin, _, at = bounds(s, b, e)
            put_rows(s, e, at, begin, new[e * WINDOW:(e + 1) * WINDOW, :], gates[e])

        def more(j, _):
            k, e = j // experts + 1, lax.rem(j, experts)
            begin, _, at = bounds(s, b, e)
            at = at + k * WINDOW

            @pl.when(at < jnp.minimum(base_ref[s, b + 1, e], cap))
            def _():
                pick = (local + at).astype(jnp.float32) == slot_lane[s, pl.ds(e, 1), span]
                got = jnp.sum(jnp.where(pick, gate_lane[s, pl.ds(e, 1), span], 0.0), axis=1, keepdims=True)
                new = jnp.dot(pick.astype(jnp.bfloat16), tok_ref[s, span, :], preferred_element_type=jnp.float32)
                put_rows(s, e, at, begin, new, got)

            return 0

        lax.fori_loop(0, extra_windows(s, b) * experts, more, 0)
        return 0

    lax.fori_loop(0, sources * blocks, dispatch, 0)

    def tile(e, s, buf, lo, rows):
        where = pl.ds(pl.multiple_of(e * stride + lo, 16), rows)
        x = rows_ref[s, where, :]
        for at, width in chunks_of(ff, CHUNK):
            a = jnp.dot(x, wg_buf[buf, :, at:at + width], preferred_element_type=jnp.float32)
            b = jnp.dot(x, wu_buf[buf, :, at:at + width], preferred_element_type=jnp.float32)
            h_ref[:rows, at:at + width] = (a * jax.nn.sigmoid(a) * b).astype(jnp.bfloat16)
        y = jnp.dot(h_ref[:rows, :], wd_buf[buf], preferred_element_type=jnp.float32)
        rows_ref[s, where, :] = (y * row_gate[s, where, :]).astype(jnp.bfloat16)

    def expert_step(e, _):
        buf = lax.rem(e, 2)
        for copy in weight_copies(e, buf):
            copy.wait()

        @pl.when(e + 1 < experts)
        def _():
            for copy in weight_copies(e + 1, 1 - buf):
                copy.start()

        def source_step(s, _):
            n = jnp.minimum(base_ref[s, blocks, e], cap)

            @pl.when((n > 0) & (n <= small))
            def _():
                tile(e, s, buf, 0, small)

            @pl.when(n > small)
            def _():
                tile(e, s, buf, 0, cap)

            return 0

        lax.fori_loop(0, sources, source_step, 0)
        return 0

    lax.fori_loop(0, experts, expert_step, 0)

    def combine(i, _):
        s, b = i // blocks, lax.rem(i, blocks)
        span = pl.ds(pl.multiple_of(b * BLOCK, BLOCK), BLOCK)
        local = lax.broadcasted_iota(jnp.int32, (BLOCK, WINDOW), 1)
        puts = []
        for e in range(experts):
            _, _, at = bounds(s, b, e)
            puts.append(((local + at).astype(jnp.float32) == slot_sub[s, span, e:e + 1]).astype(jnp.bfloat16))
            yblk_ref[e * WINDOW:(e + 1) * WINDOW, :] = rows_ref[s, pl.ds(pl.multiple_of(e * stride + at, 16), WINDOW), :]
        total = jnp.dot(jnp.concatenate(puts, axis=1), yblk_ref[...], preferred_element_type=jnp.float32)
        tok_ref[s, span, :] = total.astype(jnp.bfloat16)
        extra = extra_windows(s, b)

        @pl.when(extra > 0)
        def _():
            acc_ref[...] = jnp.zeros_like(acc_ref)

            def every(i, _):
                k, e = i // experts, lax.rem(i, experts)
                _, _, at = bounds(s, b, e)
                at = at + k * WINDOW

                @pl.when(at < jnp.minimum(base_ref[s, b + 1, e], cap))
                def _():
                    col = lax.broadcasted_iota(jnp.int32, (BLOCK, experts), 1)
                    mine = jnp.sum(jnp.where(col == e, slot_sub[s, span, :], 0.0), axis=1, keepdims=True)
                    put = ((local + at).astype(jnp.float32) == mine).astype(jnp.bfloat16)
                    y = rows_ref[s, pl.ds(pl.multiple_of(e * stride + at, 16), WINDOW), :]
                    acc_ref[...] += jnp.dot(put, y, preferred_element_type=jnp.float32)

                return 0

            lax.fori_loop(0, (extra + 1) * experts, every, 0)
            tok_ref[s, span, :] = acc_ref[...].astype(jnp.bfloat16)

        for t in range(sources):

            @pl.when(s == t)
            def _():
                pltpu.make_async_copy(tok_ref.at[t, span, :], out_hbm[t].at[span, :], out_sem).start()
        return 0

    lax.fori_loop(0, sources * blocks, combine, 0)
    for s in range(sources):
        pltpu.make_async_copy(tok_ref.at[s], out_hbm[s], out_sem).wait()


def phase(routes, toks, wg, wu, wd, cap, after=()):
    sources, _, tok_dev = routes.shape
    d_model = toks[0].shape[1]
    experts, _, ff = wg.shape
    small = min(cap, 256)
    vm = pl.BlockSpec(memory_space=pltpu.VMEM)
    hbm = pl.BlockSpec(memory_space=pl.ANY)
    blocks = tok_dev // BLOCK
    height = experts * (cap + WINDOW)
    return pl.pallas_call(
        functools.partial(phase_kernel, cap, small, len(toks), len(after)),
        out_shape=[jax.ShapeDtypeStruct((tok_dev, d_model), jnp.bfloat16)] * sources,
        in_specs=[vm] + [hbm] * (len(toks) + 3 + len(after)),
        out_specs=[hbm] * sources,
        scratch_shapes=[
            pltpu.VMEM((2, d_model, ff), jnp.bfloat16),
            pltpu.VMEM((2, d_model, ff), jnp.bfloat16),
            pltpu.VMEM((2, ff, d_model), jnp.bfloat16),
            pltpu.VMEM((sources, tok_dev, d_model), jnp.bfloat16),
            pltpu.VMEM((sources, height, d_model), jnp.bfloat16),
            pltpu.VMEM((experts * WINDOW, BLOCK), jnp.bfloat16),
            pltpu.VMEM((experts * WINDOW, d_model), jnp.bfloat16),
            pltpu.VMEM((BLOCK, d_model), jnp.float32),
            pltpu.VMEM((sources, experts, tok_dev), jnp.float32),
            pltpu.VMEM((sources, experts, tok_dev), jnp.float32),
            pltpu.VMEM((sources, tok_dev, experts), jnp.float32),
            pltpu.VMEM((sources, height, 1), jnp.float32),
            pltpu.VMEM((cap, ff), jnp.bfloat16),
            pltpu.SMEM((sources, blocks + 1, experts), jnp.int32),
            pltpu.SemaphoreType.DMA((2, 3 * PARTS)),
            pltpu.SemaphoreType.DMA((len(toks),)),
            pltpu.SemaphoreType.DMA,
        ],
        compiler_params=pltpu.CompilerParams(vmem_limit_bytes=60 * 2**20),
        cost_estimate=pl.CostEstimate(
            flops=6 * sources * experts * small * d_model * ff,
            bytes_accessed=6 * experts * d_model * ff,
            transcendentals=0,
        ),
        name="moe_phase",
    )(routes, *toks, wg, wu, wd, *after)


def solution(mesh):
    ep_size = mesh.shape["ep"]
    tp_size = mesh.shape["tp"]
    row_spec = P(("dp", "ep", "tp"), None)
    axes = ("dp", "ep", "tp")
    ranks = [(d, y, t) for d in range(mesh.shape["dp"]) for y in range(ep_size) for t in range(tp_size)]

    def rank_of(d, y, t):
        return (d * ep_size + y) * tp_size + t

    def shift(arr, flip_ep, flip_tp):
        return lax.ppermute(arr, axes, [(rank_of(*r), rank_of(r[0], r[1] ^ flip_ep, r[2] ^ flip_tp)) for r in ranks])

    def local_layer(tokens, expert_ids, gates, w_gate, w_up, w_down):
        tok_dev, _ = tokens.shape
        top_k = expert_ids.shape[1]
        local_experts = w_gate.shape[0]
        capacity = 5 * top_k * tok_dev // (4 * local_experts * ep_size)
        first = (lax.axis_index("ep") * local_experts).astype(jnp.float32)
        routes = jnp.concatenate([expert_ids.T.astype(jnp.float32), gates.T], axis=0)
        half = tok_dev // 2

        def run(tok_list, route_list, *after):
            stacked = jnp.stack(route_list)
            lines = jnp.arange(2 * top_k)[None, :, None] < top_k
            stacked = jnp.where(lines, stacked - first, stacked)
            return phase(stacked, tok_list, w_gate, w_up, w_down, capacity, after)

        r_x, r_y, t_x, t_y = shift(routes, 0, 2), shift(routes, 1, 0), shift(tokens, 0, 2), shift(tokens, 1, 0)
        (own,) = run([tokens], [routes])
        r_x, r_y, t_x, t_y, own, mine, mine_r = lax.optimization_barrier((r_x, r_y, t_x, t_y, own, tokens, routes))
        r_xp, t_xp = shift(r_x, 0, 1), shift(t_x, 0, 1)
        r_yp, t_yp = shift(r_y, 0, 1), shift(t_y, 0, 1)
        r_d, d_lo, d_hi = shift(r_x, 1, 0), shift(t_x[:half], 1, 0), shift(t_y[half:], 0, 2)
        t_p, r_p = shift(mine, 0, 1), shift(mine_r, 0, 1)
        x_a, x_b = run([t_x, t_xp], [r_x, r_xp], own)
        x_in = shift(x_b, 0, 1)
        r_d, d_lo, d_hi, _ = lax.optimization_barrier((r_d, d_lo, d_hi, x_a))
        r_dp, p_lo, p_hi = shift(r_d, 0, 1), shift(d_lo, 0, 1), shift(d_hi, 0, 1)
        y_a, y_b = run([t_y, t_yp], [r_y, r_yp], x_a)
        x_sum = add_pair(x_a, x_in)
        x_back = shift(x_sum, 0, 2)
        y_in = shift(y_b, 0, 1)
        d_a, d_b = run([d_lo, d_hi, p_lo, p_hi], [r_d, r_dp], x_sum, y_a, t_p, r_p)
        d_in = shift(d_b, 0, 1)
        y_sum = add_pair(y_a, y_in)
        y_back = shift(y_sum, 1, 0)
        d_sum = add_pair(d_a, d_in)
        d_back = shift(d_sum, 1, 2)
        (part,) = run([t_p], [r_p], y_sum, d_sum)
        p_back = shift(part, 0, 1)
        total = own.astype(jnp.float32)
        for piece in (p_back, x_back, y_back, d_back):
            total += piece.astype(jnp.float32)
        return total.astype(jnp.bfloat16)

    return jax.shard_map(
        local_layer,
        mesh=mesh,
        in_specs=(row_spec, row_spec, row_spec, P("ep", None, "tp"), P("ep", None, "tp"), P("ep", "tp", None)),
        out_specs=row_spec,
        check_vma=False,
    )
```

```python
import functools
import jax
import jax.numpy as jnp
from jax import lax
from jax.experimental import pallas as pl
from jax.experimental.pallas import tpu as pltpu

from jax.sharding import PartitionSpec as P


def add_pair(a, b):
    return (a.astype(jnp.float32) + b.astype(jnp.float32)).astype(jnp.bfloat16)


CHUNK = 512
BLOCK = 256
PARTS = 3
WINDOW = 128


def chunks_of(width, step):
    return [(lo, min(step, width - lo)) for lo in range(0, width, step)]


def phase_kernel(cap, small, first, experts, pieces, adds, waits, route_ref, *refs):
    tok_hbm, refs = refs[:pieces], refs[pieces:]
    wg_hbm, wu_hbm, wd_hbm = refs[:3]
    add_hbm = refs[3:3 + adds]
    refs = refs[3 + adds + waits:]
    sources, lines, toks = route_ref.shape
    out_hbm = refs[:sources]
    (wg_buf, wu_buf, wd_buf, tok_ref, rows_ref, pick_ref, yblk_ref, yblk2_ref, acc_ref, slot_lane, gate_lane, slot_sub, row_gate, h_ref,
     base_ref, sems, tok_sems, out_sem, *sum_refs) = refs[sources:]
    top_k = lines // 2
    ff = wg_hbm.shape[2]
    blocks = toks // BLOCK
    stride = cap + WINDOW

    def weight_copies(e, buf):
        copies = []
        for i, (src, dst) in enumerate(((wg_hbm, wg_buf), (wu_hbm, wu_buf), (wd_hbm, wd_buf))):
            rows = src.shape[1] // PARTS
            for p in range(PARTS):
                part = pl.ds(p * rows, rows)
                copies.append(pltpu.make_async_copy(src.at[first + e, part, :], dst.at[buf, part, :], sems.at[buf, i * PARTS + p]))
        return copies

    size = sources * toks // pieces
    tok_copies = [
        pltpu.make_async_copy(tok_hbm[p], tok_ref.at[p * size // toks, pl.ds(p * size % toks, size), :], tok_sems.at[p])
        for p in range(pieces)
    ]
    for copy in tok_copies:
        copy.start()

    tri = (lax.broadcasted_iota(jnp.int32, (128, 128), 0) < lax.broadcasted_iota(jnp.int32, (128, 128), 1)).astype(jnp.bfloat16)
    expert_row = (lax.broadcasted_iota(jnp.int32, (experts, toks), 0) + first).astype(jnp.float32)

    def number(s, _):
        hit = jnp.zeros((experts, toks), jnp.float32)
        gate = jnp.zeros((experts, toks), jnp.float32)
        for j in range(top_k):
            same = route_ref[s, j:j + 1, :] == expert_row
            hit = jnp.where(same, 1.0, hit)
            gate = jnp.where(same, route_ref[s, top_k + j:top_k + j + 1, :], gate)
        lanes = [hit[:, lo:lo + 128] for lo in range(0, toks, 128)]
        inner = jnp.dot(jnp.concatenate(lanes, axis=0).astype(jnp.bfloat16), tri, preferred_element_type=jnp.float32)
        base = jnp.zeros((experts, 1), jnp.float32)
        parts = []
        for i in range(len(lanes)):
            if i * 128 % BLOCK == 0:
                for e in range(experts):
                    base_ref[s, i * 128 // BLOCK, e] = base[e, 0].astype(jnp.int32)
            part = inner[i * experts:(i + 1) * experts, :]
            parts.append(part + base)
            base = base + part[:, 127:128] + lanes[i][:, 127:128]
        for e in range(experts):
            base_ref[s, blocks, e] = base[e, 0].astype(jnp.int32)
        slot = jnp.concatenate(parts, axis=1)
        slot = jnp.where((hit > 0) & (slot < cap), slot, -1.0)
        slot_lane[s] = slot
        gate_lane[s] = gate
        slot_sub[s] = jnp.transpose(slot)
        return 0

    lax.fori_loop(0, sources, number, 0)
    rows_ref[...] = jnp.zeros_like(rows_ref)
    row_gate[...] = jnp.zeros_like(row_gate)
    for copy in tok_copies:
        copy.wait()
    for copy in weight_copies(0, 0):
        copy.start()
    if adds:
        add_ref, sum_ref, add_sem = sum_refs
        add_copies = [pltpu.make_async_copy(add_hbm[i], add_ref.at[i], add_sem.at[i]) for i in range(adds)]
        for copy in add_copies:
            copy.start()

    def bounds(s, b, e):
        begin = jnp.minimum(base_ref[s, b, e], cap)
        end = jnp.minimum(base_ref[s, b + 1, e], cap)
        return begin, end, (begin // 16) * 16

    def extra_windows(s, b):
        most = jnp.int32(0)
        for e in range(experts):
            _, end, at = bounds(s, b, e)
            most = jnp.maximum(most, end - at)
        return jnp.maximum(most - 1, 0) // WINDOW

    def put_rows(s, e, at, begin, new, gates):
        head = pl.ds(pl.multiple_of(e * stride + at, 16), 16)
        rest = pl.ds(pl.multiple_of(e * stride + at + 16, 16), WINDOW - 16)
        old = lax.broadcasted_iota(jnp.int32, (16, 1), 0) + at < begin
        rows_ref[s, head, :] = jnp.where(old, rows_ref[s, head, :].astype(jnp.float32), new[:16]).astype(jnp.bfloat16)
        row_gate[s, head, :] = jnp.where(old, row_gate[s, head, :], gates[:16])
        rows_ref[s, rest, :] = new[16:].astype(jnp.bfloat16)
        row_gate[s, rest, :] = gates[16:]

    def dispatch(i, _):
        s, b = i // blocks, lax.rem(i, blocks)
        span = pl.ds(pl.multiple_of(b * BLOCK, BLOCK), BLOCK)
        local = lax.broadcasted_iota(jnp.int32, (WINDOW, BLOCK), 0)

        def one_hot(e, at):
            return (local + at).astype(jnp.float32) == slot_lane[s, e:e + 1, span]

        def gates_of(pick, e):
            return jnp.sum(jnp.where(pick, gate_lane[s, e:e + 1, span], 0.0), axis=1, keepdims=True)

        gates = []
        for e in range(experts):
            _, _, at = bounds(s, b, e)
            pick = one_hot(e, at)
            gates.append(gates_of(pick, e))
            pick_ref[e * WINDOW:(e + 1) * WINDOW, :] = pick.astype(jnp.bfloat16)
        new = jnp.dot(pick_ref[...], tok_ref[s, span, :], preferred_element_type=jnp.float32)
        for e in range(experts):
            begin, _, at = bounds(s, b, e)
            put_rows(s, e, at, begin, new[e * WINDOW:(e + 1) * WINDOW, :], gates[e])

        def more(j, _):
            k, e = j // experts + 1, lax.rem(j, experts)
            begin, _, at = bounds(s, b, e)
            at = at + k * WINDOW

            @pl.when(at < jnp.minimum(base_ref[s, b + 1, e], cap))
            def _():
                pick = (local + at).astype(jnp.float32) == slot_lane[s, pl.ds(e, 1), span]
                got = jnp.sum(jnp.where(pick, gate_lane[s, pl.ds(e, 1), span], 0.0), axis=1, keepdims=True)
                new = jnp.dot(pick.astype(jnp.bfloat16), tok_ref[s, span, :], preferred_element_type=jnp.float32)
                put_rows(s, e, at, begin, new, got)

            return 0

        lax.fori_loop(0, extra_windows(s, b) * experts, more, 0)
        return 0

    lax.fori_loop(0, sources * blocks, dispatch, 0)

    def tile(e, s, buf, lo, rows):
        where = pl.ds(pl.multiple_of(e * stride + lo, 16), rows)
        x = rows_ref[s, where, :]
        for at, width in chunks_of(ff, CHUNK):
            a = jnp.dot(x, wg_buf[buf, :, at:at + width], preferred_element_type=jnp.float32)
            b = jnp.dot(x, wu_buf[buf, :, at:at + width], preferred_element_type=jnp.float32)
            h_ref[:rows, at:at + width] = (a * jax.nn.sigmoid(a) * b).astype(jnp.bfloat16)
        y = jnp.dot(h_ref[:rows, :], wd_buf[buf], preferred_element_type=jnp.float32)
        rows_ref[s, where, :] = (y * row_gate[s, where, :]).astype(jnp.bfloat16)

    def expert_step(e, _):
        buf = lax.rem(e, 2)
        for copy in weight_copies(e, buf):
            copy.wait()

        @pl.when(e + 1 < experts)
        def _():
            for copy in weight_copies(e + 1, 1 - buf):
                copy.start()

        def source_step(s, _):
            n = jnp.minimum(base_ref[s, blocks, e], cap)

            @pl.when((n > 0) & (n <= small))
            def _():
                tile(e, s, buf, 0, small)

            @pl.when(n > small)
            def _():
                tile(e, s, buf, 0, cap)

            return 0

        lax.fori_loop(0, sources, source_step, 0)
        return 0

    lax.fori_loop(0, experts, expert_step, 0)

    def gather_rows(i, y_ref):
        s, b = i // blocks, lax.rem(i, blocks)
        span = pl.ds(pl.multiple_of(b * BLOCK, BLOCK), BLOCK)
        local = lax.broadcasted_iota(jnp.int32, (BLOCK, WINDOW), 1)
        puts = []
        for e in range(experts):
            _, _, at = bounds(s, b, e)
            puts.append(((local + at).astype(jnp.float32) == slot_sub[s, span, e:e + 1]).astype(jnp.bfloat16))
            y_ref[e * WINDOW:(e + 1) * WINDOW, :] = rows_ref[s, pl.ds(pl.multiple_of(e * stride + at, 16), WINDOW), :]
        return jnp.concatenate(puts, axis=1)

    def combine(i, put, y_ref):
        s, b = i // blocks, lax.rem(i, blocks)
        span = pl.ds(pl.multiple_of(b * BLOCK, BLOCK), BLOCK)
        total = jnp.dot(put, y_ref[...], preferred_element_type=jnp.float32)
        tok_ref[s, span, :] = total.astype(jnp.bfloat16)
        if adds:
            acc_ref[...] = total

    def finish(i):
        s, b = i // blocks, lax.rem(i, blocks)
        span = pl.ds(pl.multiple_of(b * BLOCK, BLOCK), BLOCK)
        local = lax.broadcasted_iota(jnp.int32, (BLOCK, WINDOW), 1)
        extra = extra_windows(s, b)

        @pl.when(extra > 0)
        def _():
            acc_ref[...] = jnp.zeros_like(acc_ref)

            def every(i, _):
                k, e = i // experts, lax.rem(i, experts)
                _, _, at = bounds(s, b, e)
                at = at + k * WINDOW

                @pl.when(at < jnp.minimum(base_ref[s, b + 1, e], cap))
                def _():
                    col = lax.broadcasted_iota(jnp.int32, (BLOCK, experts), 1)
                    mine = jnp.sum(jnp.where(col == e, slot_sub[s, span, :], 0.0), axis=1, keepdims=True)
                    put = ((local + at).astype(jnp.float32) == mine).astype(jnp.bfloat16)
                    y = rows_ref[s, pl.ds(pl.multiple_of(e * stride + at, 16), WINDOW), :]
                    acc_ref[...] += jnp.dot(put, y, preferred_element_type=jnp.float32)

                return 0

            lax.fori_loop(0, (extra + 1) * experts, every, 0)
            tok_ref[s, span, :] = acc_ref[...].astype(jnp.bfloat16)

        if adds:

            @pl.when(s == 0)
            def _():
                rows = acc_ref[...]
                for k in range(adds):
                    rows += add_ref[k, span, :].astype(jnp.float32)
                sum_ref[span, :] = rows
                pltpu.make_async_copy(sum_ref.at[span, :], out_hbm[0].at[span, :], out_sem).start()

        for t in range(1 if adds else 0, sources):

            @pl.when(s == t)
            def _():
                pltpu.make_async_copy(tok_ref.at[t, span, :], out_hbm[t].at[span, :], out_sem).start()

    if adds:
        for copy in add_copies:
            copy.wait()

    def pair(j, _):
        put_a = gather_rows(2 * j, yblk_ref)
        put_b = gather_rows(2 * j + 1, yblk2_ref)
        combine(2 * j, put_a, yblk_ref)
        if adds:
            finish(2 * j)
        combine(2 * j + 1, put_b, yblk2_ref)
        if not adds:
            finish(2 * j)
        finish(2 * j + 1)
        return 0

    lax.fori_loop(0, sources * blocks // 2, pair, 0)
    for s in range(sources):
        src = sum_ref if adds and s == 0 else tok_ref.at[s]
        pltpu.make_async_copy(src, out_hbm[s], out_sem).wait()


def phase(routes, toks, wg, wu, wd, cap, first=0, experts=None, adds=(), after=()):
    sources, _, tok_dev = routes.shape
    d_model = toks[0].shape[1]
    ff = wg.shape[2]
    experts = experts or wg.shape[0]
    small = min(cap, 256)
    vm = pl.BlockSpec(memory_space=pltpu.VMEM)
    hbm = pl.BlockSpec(memory_space=pl.ANY)
    blocks = tok_dev // BLOCK
    height = experts * (cap + WINDOW)
    sum_scratch = [
        pltpu.VMEM((len(adds), tok_dev, d_model), jnp.bfloat16),
        pltpu.VMEM((tok_dev, d_model), jnp.float32),
        pltpu.SemaphoreType.DMA((len(adds),)),
    ] if adds else []
    return pl.pallas_call(
        functools.partial(phase_kernel, cap, small, first, experts, len(toks), len(adds), len(after)),
        out_shape=[
            jax.ShapeDtypeStruct((tok_dev, d_model), jnp.float32 if adds and s == 0 else jnp.bfloat16) for s in range(sources)
        ],
        in_specs=[vm] + [hbm] * (len(toks) + 3 + len(adds) + len(after)),
        out_specs=[hbm] * sources,
        scratch_shapes=[
            pltpu.VMEM((2, d_model, ff), jnp.bfloat16),
            pltpu.VMEM((2, d_model, ff), jnp.bfloat16),
            pltpu.VMEM((2, ff, d_model), jnp.bfloat16),
            pltpu.VMEM((sources, tok_dev, d_model), jnp.bfloat16),
            pltpu.VMEM((sources, height, d_model), jnp.bfloat16),
            pltpu.VMEM((experts * WINDOW, BLOCK), jnp.bfloat16),
            pltpu.VMEM((experts * WINDOW, d_model), jnp.bfloat16),
            pltpu.VMEM((experts * WINDOW, d_model), jnp.bfloat16),
            pltpu.VMEM((BLOCK, d_model), jnp.float32),
            pltpu.VMEM((sources, experts, tok_dev), jnp.float32),
            pltpu.VMEM((sources, experts, tok_dev), jnp.float32),
            pltpu.VMEM((sources, tok_dev, experts), jnp.float32),
            pltpu.VMEM((sources, height, 1), jnp.float32),
            pltpu.VMEM((cap, ff), jnp.bfloat16),
            pltpu.SMEM((sources, blocks + 1, experts), jnp.int32),
            pltpu.SemaphoreType.DMA((2, 3 * PARTS)),
            pltpu.SemaphoreType.DMA((len(toks),)),
            pltpu.SemaphoreType.DMA,
        ] + sum_scratch,
        compiler_params=pltpu.CompilerParams(vmem_limit_bytes=60 * 2**20),
        cost_estimate=pl.CostEstimate(
            flops=6 * sources * experts * small * d_model * ff,
            bytes_accessed=6 * experts * d_model * ff,
            transcendentals=0,
        ),
        name="moe_phase",
    )(routes, *toks, wg, wu, wd, *adds, *after)


def solution(mesh):
    ep_size = mesh.shape["ep"]
    tp_size = mesh.shape["tp"]
    row_spec = P(("dp", "ep", "tp"), None)
    axes = ("dp", "ep", "tp")
    ranks = [(d, y, t) for d in range(mesh.shape["dp"]) for y in range(ep_size) for t in range(tp_size)]

    def rank_of(d, y, t):
        return (d * ep_size + y) * tp_size + t

    def shift(arr, flip_ep, flip_tp):
        return lax.ppermute(arr, axes, [(rank_of(*r), rank_of(r[0], r[1] ^ flip_ep, r[2] ^ flip_tp)) for r in ranks])

    def local_layer(tokens, expert_ids, gates, w_gate, w_up, w_down):
        tok_dev, _ = tokens.shape
        top_k = expert_ids.shape[1]
        local_experts = w_gate.shape[0]
        capacity = 5 * top_k * tok_dev // (4 * local_experts * ep_size)
        first = (lax.axis_index("ep") * local_experts).astype(jnp.float32)
        routes = jnp.concatenate([expert_ids.T.astype(jnp.float32), gates.T], axis=0)

        def run(tok_list, route_list, after=(), **part):
            stacked = jnp.stack(route_list)
            lines = jnp.arange(2 * top_k)[None, :, None] < top_k
            stacked = jnp.where(lines, stacked - first, stacked)
            return phase(stacked, tok_list, w_gate, w_up, w_down, capacity, after=after, **part)

        t_p, r_p = shift(tokens, 0, 1), shift(routes, 0, 1)
        r_x, r_y, t_x, t_y = shift(routes, 0, 2), shift(routes, 1, 0), shift(tokens, 0, 2), shift(tokens, 1, 0)
        own, own_p = run([tokens, t_p], [routes, r_p], experts=local_experts // 2)
        p_back = shift(own_p, 0, 1)
        r_x, r_y, t_x, t_y, own = lax.optimization_barrier((r_x, r_y, t_x, t_y, own))
        r_xp, t_xp = shift(r_x, 0, 1), shift(t_x, 0, 1)
        r_yp, t_yp = shift(r_y, 0, 1), shift(t_y, 0, 1)
        r_d, t_d = shift(r_x, 1, 0), shift(t_x, 1, 0)
        x_a, x_b = run([t_x, t_xp], [r_x, r_xp], after=(own,))
        x_back = shift(x_a, 0, 2)
        xp_back = shift(x_b, 0, 3)
        r_d, t_d, _ = lax.optimization_barrier((r_d, t_d, x_a))
        r_dp, t_dp = shift(r_d, 0, 1), shift(t_d, 0, 1)
        y_a, y_b = run([t_y, t_yp], [r_y, r_yp], after=(x_a,))
        y_back = shift(y_a, 1, 0)
        yp_back = shift(y_b, 1, 1)
        d_a, d_b = run([t_d, t_dp], [r_d, r_dp], after=(y_a,))
        d_in = shift(d_b, 0, 1)
        d_sum = add_pair(d_a, d_in)
        d_back = shift(d_sum, 1, 2)
        rest, rest_p = run(
            [tokens, t_p],
            [routes, r_p],
            after=(d_sum,),
            first=local_experts // 2,
            experts=local_experts // 2,
            adds=(own, p_back, x_back, xp_back, y_back, yp_back),
        )
        rest_back = shift(rest_p, 0, 1)
        total = rest + rest_back.astype(jnp.float32) + d_back.astype(jnp.float32)
        return total.astype(jnp.bfloat16)

    return jax.shard_map(
        local_layer,
        mesh=mesh,
        in_specs=(row_spec, row_spec, row_spec, P("ep", None, "tp"), P("ep", None, "tp"), P("ep", "tp", None)),
        out_specs=row_spec,
        check_vma=False,
    )
```

```python
import functools
import jax
import jax.numpy as jnp
from jax import lax
from jax.experimental import pallas as pl
from jax.experimental.pallas import tpu as pltpu

from jax.sharding import PartitionSpec as P


def add_pair(a, b):
    return (a.astype(jnp.float32) + b.astype(jnp.float32)).astype(jnp.bfloat16)


CHUNK = 512
BLOCK = 256
PARTS = 3
WINDOW = 128


def chunks_of(width, step):
    return [(lo, min(step, width - lo)) for lo in range(0, width, step)]


def phase_kernel(cap, small, first, experts, pieces, adds, waits, route_ref, *refs):
    tok_hbm, refs = refs[:pieces], refs[pieces:]
    wg_hbm, wu_hbm, wd_hbm = refs[:3]
    add_hbm = refs[3:3 + adds]
    refs = refs[3 + adds + waits:]
    sources, lines, toks = route_ref.shape
    out_hbm = refs[:sources]
    (wg_buf, wu_buf, wx_buf, wd_buf, tok_ref, rows_ref, pick_ref, yblk_ref, yblk2_ref, acc_ref, slot_lane, gate_lane, slot_sub, row_gate, h_ref,
     base_ref, sems, tok_sems, out_sem, *sum_refs) = refs[sources:]
    d_model = tok_ref.shape[2]
    top_k = lines // 2
    ff = wg_hbm.shape[2]
    blocks = toks // BLOCK
    stride = cap + WINDOW
    main = wg_buf.shape[2]

    def weight_copies(e, buf):
        at = first + e
        pairs = []
        for lo, rows in chunks_of(d_model, d_model // PARTS):
            part = pl.ds(lo, rows)
            pairs.append((wg_hbm.at[at, part, :main], wg_buf.at[buf, part, :]))
            pairs.append((wu_hbm.at[at, part, :main], wu_buf.at[buf, part, :]))
        if main < ff:
            pairs.append((wg_hbm.at[at, :, main:], wx_buf.at[buf, :, :ff - main]))
            pairs.append((wu_hbm.at[at, :, main:], wx_buf.at[buf, :, ff - main:]))
        for lo, rows in chunks_of(ff, ff // PARTS):
            pairs.append((wd_hbm.at[at, pl.ds(lo, rows), :], wd_buf.at[buf, pl.ds(lo, rows), :]))
        return [pltpu.make_async_copy(src, dst, sems.at[buf, i]) for i, (src, dst) in enumerate(pairs)]

    size = sources * toks // pieces
    tok_copies = [
        pltpu.make_async_copy(tok_hbm[p], tok_ref.at[p * size // toks, pl.ds(p * size % toks, size), :], tok_sems.at[p])
        for p in range(pieces)
    ]
    for copy in tok_copies:
        copy.start()

    tri = (lax.broadcasted_iota(jnp.int32, (128, 128), 0) < lax.broadcasted_iota(jnp.int32, (128, 128), 1)).astype(jnp.bfloat16)
    expert_row = (lax.broadcasted_iota(jnp.int32, (experts, toks), 0) + first).astype(jnp.float32)

    def number(s, _):
        hit = jnp.zeros((experts, toks), jnp.float32)
        gate = jnp.zeros((experts, toks), jnp.float32)
        for j in range(top_k):
            same = route_ref[s, j:j + 1, :] == expert_row
            hit = jnp.where(same, 1.0, hit)
            gate = jnp.where(same, route_ref[s, top_k + j:top_k + j + 1, :], gate)
        lanes = [hit[:, lo:lo + 128] for lo in range(0, toks, 128)]
        inner = jnp.dot(jnp.concatenate(lanes, axis=0).astype(jnp.bfloat16), tri, preferred_element_type=jnp.float32)
        base = jnp.zeros((experts, 1), jnp.float32)
        parts = []
        for i in range(len(lanes)):
            if i * 128 % BLOCK == 0:
                for e in range(experts):
                    base_ref[s, i * 128 // BLOCK, e] = base[e, 0].astype(jnp.int32)
            part = inner[i * experts:(i + 1) * experts, :]
            parts.append(part + base)
            base = base + part[:, 127:128] + lanes[i][:, 127:128]
        for e in range(experts):
            base_ref[s, blocks, e] = base[e, 0].astype(jnp.int32)
        slot = jnp.concatenate(parts, axis=1)
        slot = jnp.where((hit > 0) & (slot < cap), slot, -1.0)
        slot_lane[s] = slot
        gate_lane[s] = gate
        slot_sub[s] = jnp.transpose(slot)
        return 0

    lax.fori_loop(0, sources, number, 0)
    rows_ref[...] = jnp.zeros_like(rows_ref)
    row_gate[...] = jnp.zeros_like(row_gate)
    for copy in tok_copies:
        copy.wait()
    for copy in weight_copies(0, 0):
        copy.start()
    if adds:
        add_ref, sum_ref, add_sem = sum_refs
        add_copies = [pltpu.make_async_copy(add_hbm[i], add_ref.at[i], add_sem.at[i]) for i in range(adds)]
        for copy in add_copies:
            copy.start()

    def bounds(s, b, e):
        begin = jnp.minimum(base_ref[s, b, e], cap)
        end = jnp.minimum(base_ref[s, b + 1, e], cap)
        return begin, end, (begin // 16) * 16

    def extra_windows(s, b):
        most = jnp.int32(0)
        for e in range(experts):
            _, end, at = bounds(s, b, e)
            most = jnp.maximum(most, end - at)
        return jnp.maximum(most - 1, 0) // WINDOW

    def put_rows(s, e, at, begin, new, gates):
        head = pl.ds(pl.multiple_of(e * stride + at, 16), 16)
        rest = pl.ds(pl.multiple_of(e * stride + at + 16, 16), WINDOW - 16)
        old = lax.broadcasted_iota(jnp.int32, (16, 1), 0) + at < begin
        rows_ref[s, head, :] = jnp.where(old, rows_ref[s, head, :].astype(jnp.float32), new[:16]).astype(jnp.bfloat16)
        row_gate[s, head, :] = jnp.where(old, row_gate[s, head, :], gates[:16])
        rows_ref[s, rest, :] = new[16:].astype(jnp.bfloat16)
        row_gate[s, rest, :] = gates[16:]

    def dispatch(i, _):
        s, b = i // blocks, lax.rem(i, blocks)
        span = pl.ds(pl.multiple_of(b * BLOCK, BLOCK), BLOCK)
        local = lax.broadcasted_iota(jnp.int32, (WINDOW, BLOCK), 0)

        def one_hot(e, at):
            return (local + at).astype(jnp.float32) == slot_lane[s, e:e + 1, span]

        def gates_of(pick, e):
            return jnp.sum(jnp.where(pick, gate_lane[s, e:e + 1, span], 0.0), axis=1, keepdims=True)

        gates = []
        for e in range(experts):
            _, _, at = bounds(s, b, e)
            pick = one_hot(e, at)
            gates.append(gates_of(pick, e))
            pick_ref[e * WINDOW:(e + 1) * WINDOW, :] = pick.astype(jnp.bfloat16)
        new = jnp.dot(pick_ref[...], tok_ref[s, span, :], preferred_element_type=jnp.float32)
        for e in range(experts):
            begin, _, at = bounds(s, b, e)
            put_rows(s, e, at, begin, new[e * WINDOW:(e + 1) * WINDOW, :], gates[e])

        def more(j, _):
            k, e = j // experts + 1, lax.rem(j, experts)
            begin, _, at = bounds(s, b, e)
            at = at + k * WINDOW

            @pl.when(at < jnp.minimum(base_ref[s, b + 1, e], cap))
            def _():
                pick = (local + at).astype(jnp.float32) == slot_lane[s, pl.ds(e, 1), span]
                got = jnp.sum(jnp.where(pick, gate_lane[s, pl.ds(e, 1), span], 0.0), axis=1, keepdims=True)
                new = jnp.dot(pick.astype(jnp.bfloat16), tok_ref[s, span, :], preferred_element_type=jnp.float32)
                put_rows(s, e, at, begin, new, got)

            return 0

        lax.fori_loop(0, extra_windows(s, b) * experts, more, 0)
        return 0

    lax.fori_loop(0, sources * blocks, dispatch, 0)

    def tile(e, s, buf, lo, rows):
        where = pl.ds(pl.multiple_of(e * stride + lo, 16), rows)
        x = rows_ref[s, where, :]
        for at, width in chunks_of(main, CHUNK):
            a = jnp.dot(x, wg_buf[buf, :, at:at + width], preferred_element_type=jnp.float32)
            b = jnp.dot(x, wu_buf[buf, :, at:at + width], preferred_element_type=jnp.float32)
            h_ref[:rows, at:at + width] = (a * jax.nn.sigmoid(a) * b).astype(jnp.bfloat16)
        if main < ff:
            ab = jnp.dot(x, wx_buf[buf], preferred_element_type=jnp.float32)
            a, b = ab[:, :ff - main], ab[:, ff - main:]
            h_ref[:rows, main:] = (a * jax.nn.sigmoid(a) * b).astype(jnp.bfloat16)
        y = jnp.dot(h_ref[:rows, :], wd_buf[buf], preferred_element_type=jnp.float32)
        rows_ref[s, where, :] = (y * row_gate[s, where, :]).astype(jnp.bfloat16)

    def expert_step(e, _):
        buf = lax.rem(e, 2)
        for copy in weight_copies(e, buf):
            copy.wait()

        @pl.when(e + 1 < experts)
        def _():
            for copy in weight_copies(e + 1, 1 - buf):
                copy.start()

        def source_step(s, _):
            n = jnp.minimum(base_ref[s, blocks, e], cap)

            @pl.when(n > 0)
            def _():
                tile(e, s, buf, 0, small)

            if cap > small:

                @pl.when(n > small)
                def _():
                    tile(e, s, buf, small, cap - small)
            return 0

        lax.fori_loop(0, sources, source_step, 0)
        return 0

    lax.fori_loop(0, experts, expert_step, 0)

    def gather_rows(i, y_ref):
        s, b = i // blocks, lax.rem(i, blocks)
        span = pl.ds(pl.multiple_of(b * BLOCK, BLOCK), BLOCK)
        local = lax.broadcasted_iota(jnp.int32, (BLOCK, WINDOW), 1)
        puts = []
        for e in range(experts):
            _, _, at = bounds(s, b, e)
            puts.append(((local + at).astype(jnp.float32) == slot_sub[s, span, e:e + 1]).astype(jnp.bfloat16))
            y_ref[e * WINDOW:(e + 1) * WINDOW, :] = rows_ref[s, pl.ds(pl.multiple_of(e * stride + at, 16), WINDOW), :]
        return jnp.concatenate(puts, axis=1)

    def combine(i, put, y_ref):
        s, b = i // blocks, lax.rem(i, blocks)
        span = pl.ds(pl.multiple_of(b * BLOCK, BLOCK), BLOCK)
        total = jnp.dot(put, y_ref[...], preferred_element_type=jnp.float32)
        tok_ref[s, span, :] = total.astype(jnp.bfloat16)
        if adds:
            acc_ref[...] = total

    def finish(i):
        s, b = i // blocks, lax.rem(i, blocks)
        span = pl.ds(pl.multiple_of(b * BLOCK, BLOCK), BLOCK)
        local = lax.broadcasted_iota(jnp.int32, (BLOCK, WINDOW), 1)
        extra = extra_windows(s, b)

        @pl.when(extra > 0)
        def _():
            acc_ref[...] = jnp.zeros_like(acc_ref)

            def every(i, _):
                k, e = i // experts, lax.rem(i, experts)
                _, _, at = bounds(s, b, e)
                at = at + k * WINDOW

                @pl.when(at < jnp.minimum(base_ref[s, b + 1, e], cap))
                def _():
                    col = lax.broadcasted_iota(jnp.int32, (BLOCK, experts), 1)
                    mine = jnp.sum(jnp.where(col == e, slot_sub[s, span, :], 0.0), axis=1, keepdims=True)
                    put = ((local + at).astype(jnp.float32) == mine).astype(jnp.bfloat16)
                    y = rows_ref[s, pl.ds(pl.multiple_of(e * stride + at, 16), WINDOW), :]
                    acc_ref[...] += jnp.dot(put, y, preferred_element_type=jnp.float32)

                return 0

            lax.fori_loop(0, (extra + 1) * experts, every, 0)
            tok_ref[s, span, :] = acc_ref[...].astype(jnp.bfloat16)

        if adds:

            @pl.when(s == 0)
            def _():
                rows = acc_ref[...]
                for k in range(adds):
                    rows += add_ref[k, span, :].astype(jnp.float32)
                sum_ref[span, :] = rows
                pltpu.make_async_copy(sum_ref.at[span, :], out_hbm[0].at[span, :], out_sem).start()

        for t in range(1 if adds else 0, sources):

            @pl.when(s == t)
            def _():
                pltpu.make_async_copy(tok_ref.at[t, span, :], out_hbm[t].at[span, :], out_sem).start()

    if adds:
        for copy in add_copies:
            copy.wait()

    def pair(j, _):
        put_a = gather_rows(2 * j, yblk_ref)
        put_b = gather_rows(2 * j + 1, yblk2_ref)
        combine(2 * j, put_a, yblk_ref)
        if adds:
            finish(2 * j)
        combine(2 * j + 1, put_b, yblk2_ref)
        if not adds:
            finish(2 * j)
        finish(2 * j + 1)
        return 0

    lax.fori_loop(0, sources * blocks // 2, pair, 0)
    for s in range(sources):
        src = sum_ref if adds and s == 0 else tok_ref.at[s]
        pltpu.make_async_copy(src, out_hbm[s], out_sem).wait()


def phase(routes, toks, wg, wu, wd, cap, first=0, experts=None, adds=(), after=()):
    sources, _, tok_dev = routes.shape
    d_model = toks[0].shape[1]
    ff = wg.shape[2]
    main = ff // 256 * 256
    experts = experts or wg.shape[0]
    small = min(cap, 256)
    vm = pl.BlockSpec(memory_space=pltpu.VMEM)
    hbm = pl.BlockSpec(memory_space=pl.ANY)
    blocks = tok_dev // BLOCK
    height = experts * (cap + WINDOW)
    sum_scratch = [
        pltpu.VMEM((len(adds), tok_dev, d_model), jnp.bfloat16),
        pltpu.VMEM((tok_dev, d_model), jnp.float32),
        pltpu.SemaphoreType.DMA((len(adds),)),
    ] if adds else []
    return pl.pallas_call(
        functools.partial(phase_kernel, cap, small, first, experts, len(toks), len(adds), len(after)),
        out_shape=[
            jax.ShapeDtypeStruct((tok_dev, d_model), jnp.float32 if adds and s == 0 else jnp.bfloat16) for s in range(sources)
        ],
        in_specs=[vm] + [hbm] * (len(toks) + 3 + len(adds) + len(after)),
        out_specs=[hbm] * sources,
        scratch_shapes=[
            pltpu.VMEM((2, d_model, main), jnp.bfloat16),
            pltpu.VMEM((2, d_model, main), jnp.bfloat16),
            pltpu.VMEM((2, d_model, 2 * max(ff - main, 128)), jnp.bfloat16),
            pltpu.VMEM((2, ff, d_model), jnp.bfloat16),
            pltpu.VMEM((sources, tok_dev, d_model), jnp.bfloat16),
            pltpu.VMEM((sources, height, d_model), jnp.bfloat16),
            pltpu.VMEM((experts * WINDOW, BLOCK), jnp.bfloat16),
            pltpu.VMEM((experts * WINDOW, d_model), jnp.bfloat16),
            pltpu.VMEM((experts * WINDOW, d_model), jnp.bfloat16),
            pltpu.VMEM((BLOCK, d_model), jnp.float32),
            pltpu.VMEM((sources, experts, tok_dev), jnp.float32),
            pltpu.VMEM((sources, experts, tok_dev), jnp.float32),
            pltpu.VMEM((sources, tok_dev, experts), jnp.float32),
            pltpu.VMEM((sources, height, 1), jnp.float32),
            pltpu.VMEM((small, ff), jnp.bfloat16),
            pltpu.SMEM((sources, blocks + 1, experts), jnp.int32),
            pltpu.SemaphoreType.DMA((2, 3 * PARTS + 2)),
            pltpu.SemaphoreType.DMA((len(toks),)),
            pltpu.SemaphoreType.DMA,
        ] + sum_scratch,
        compiler_params=pltpu.CompilerParams(vmem_limit_bytes=67_000_000),
        cost_estimate=pl.CostEstimate(
            flops=6 * sources * experts * small * d_model * ff,
            bytes_accessed=6 * experts * d_model * ff,
            transcendentals=0,
        ),
        name="moe_phase",
    )(routes, *toks, wg, wu, wd, *adds, *after)


def solution(mesh):
    ep_size = mesh.shape["ep"]
    tp_size = mesh.shape["tp"]
    row_spec = P(("dp", "ep", "tp"), None)
    axes = ("dp", "ep", "tp")
    ranks = [(d, y, t) for d in range(mesh.shape["dp"]) for y in range(ep_size) for t in range(tp_size)]

    def rank_of(d, y, t):
        return (d * ep_size + y) * tp_size + t

    def shift(arr, flip_ep, flip_tp):
        return lax.ppermute(arr, axes, [(rank_of(*r), rank_of(r[0], r[1] ^ flip_ep, r[2] ^ flip_tp)) for r in ranks])

    def local_layer(tokens, expert_ids, gates, w_gate, w_up, w_down):
        tok_dev, _ = tokens.shape
        top_k = expert_ids.shape[1]
        local_experts = w_gate.shape[0]
        capacity = 5 * top_k * tok_dev // (4 * local_experts * ep_size)
        first = (lax.axis_index("ep") * local_experts).astype(jnp.float32)
        routes = jnp.concatenate([expert_ids.T.astype(jnp.float32), gates.T], axis=0)

        def run(tok_list, route_list, after=(), **part):
            stacked = jnp.stack(route_list)
            lines = jnp.arange(2 * top_k)[None, :, None] < top_k
            stacked = jnp.where(lines, stacked - first, stacked)
            return phase(stacked, tok_list, w_gate, w_up, w_down, capacity, after=after, **part)

        t_p, r_p = shift(tokens, 0, 1), shift(routes, 0, 1)
        r_x, r_y, t_x, t_y = shift(routes, 0, 2), shift(routes, 1, 0), shift(tokens, 0, 2), shift(tokens, 1, 0)
        own, own_p = run([tokens, t_p], [routes, r_p], experts=local_experts // 2)
        p_back = shift(own_p, 0, 1)
        r_x, r_y, t_x, t_y, own = lax.optimization_barrier((r_x, r_y, t_x, t_y, own))
        r_xp, t_xp = shift(r_x, 0, 1), shift(t_x, 0, 1)
        r_yp, t_yp = shift(r_y, 0, 1), shift(t_y, 0, 1)
        r_d, t_d = shift(r_x, 1, 0), shift(t_x, 1, 0)
        x_a, x_b = run([t_x, t_xp], [r_x, r_xp], after=(own,))
        x_back = shift(x_a, 0, 2)
        xp_back = shift(x_b, 0, 3)
        r_d, t_d, _ = lax.optimization_barrier((r_d, t_d, x_a))
        r_dp, t_dp = shift(r_d, 0, 1), shift(t_d, 0, 1)
        y_a, y_b = run([t_y, t_yp], [r_y, r_yp], after=(x_a,))
        y_back = shift(y_a, 1, 0)
        yp_back = shift(y_b, 1, 1)
        d_a, d_b = run([t_d, t_dp], [r_d, r_dp], after=(y_a,))
        d_in = shift(d_b, 0, 1)
        d_sum = add_pair(d_a, d_in)
        d_back = shift(d_sum, 1, 2)
        rest, rest_p = run(
            [tokens, t_p],
            [routes, r_p],
            after=(d_sum,),
            first=local_experts // 2,
            experts=local_experts // 2,
            adds=(own, p_back, x_back, xp_back, y_back, yp_back),
        )
        rest_back = shift(rest_p, 0, 1)
        total = rest + rest_back.astype(jnp.float32) + d_back.astype(jnp.float32)
        return total.astype(jnp.bfloat16)

    return jax.shard_map(
        local_layer,
        mesh=mesh,
        in_specs=(row_spec, row_spec, row_spec, P("ep", None, "tp"), P("ep", None, "tp"), P("ep", "tp", None)),
        out_specs=row_spec,
        check_vma=False,
    )
```

```python
import functools
import jax
import jax.numpy as jnp
from jax import lax
from jax.experimental import pallas as pl
from jax.experimental.pallas import tpu as pltpu

from jax.sharding import PartitionSpec as P


def add_pair(a, b):
    return (a.astype(jnp.float32) + b.astype(jnp.float32)).astype(jnp.bfloat16)


CHUNK = 512
BLOCK = 256
PARTS = 3
WINDOW = 128


def chunks_of(width, step):
    return [(lo, min(step, width - lo)) for lo in range(0, width, step)]


def phase_kernel(cap, small, first, experts, pieces, adds, waits, route_ref, *refs):
    tok_hbm, refs = refs[:pieces], refs[pieces:]
    wg_hbm, wu_hbm, wd_hbm = refs[:3]
    add_hbm = refs[3:3 + adds]
    refs = refs[3 + adds + waits:]
    sources, lines, toks = route_ref.shape
    out_hbm = refs[:sources]
    (wg_buf, wu_buf, wx_buf, wd_buf, tok_ref, rows_ref, pick_ref, yblk_ref, yblk2_ref, acc_ref, slot_lane, gate_lane, slot_sub, row_gate, h_ref,
     base_ref, sems, tok_sems, out_sem, *sum_refs) = refs[sources:]
    d_model = tok_ref.shape[2]
    top_k = lines // 2
    ff = wg_hbm.shape[2]
    blocks = toks // BLOCK
    stride = cap + WINDOW
    main = wg_buf.shape[2]

    def weight_copies(e, buf):
        at = first + e
        pairs = []
        for lo, rows in chunks_of(d_model, d_model // PARTS):
            part = pl.ds(lo, rows)
            pairs.append((wg_hbm.at[at, part, :main], wg_buf.at[buf, part, :]))
            pairs.append((wu_hbm.at[at, part, :main], wu_buf.at[buf, part, :]))
        if main < ff:
            pairs.append((wg_hbm.at[at, :, main:], wx_buf.at[buf, :, :ff - main]))
            pairs.append((wu_hbm.at[at, :, main:], wx_buf.at[buf, :, ff - main:]))
        for lo, rows in chunks_of(ff, ff // PARTS):
            pairs.append((wd_hbm.at[at, pl.ds(lo, rows), :], wd_buf.at[buf, pl.ds(lo, rows), :]))
        return [pltpu.make_async_copy(src, dst, sems.at[buf, i]) for i, (src, dst) in enumerate(pairs)]

    size = sources * toks // pieces
    tok_copies = [
        pltpu.make_async_copy(tok_hbm[p], tok_ref.at[p * size // toks, pl.ds(p * size % toks, size), :], tok_sems.at[p])
        for p in range(pieces)
    ]
    for copy in tok_copies:
        copy.start()

    tri = (lax.broadcasted_iota(jnp.int32, (128, 128), 0) < lax.broadcasted_iota(jnp.int32, (128, 128), 1)).astype(jnp.bfloat16)
    expert_row = (lax.broadcasted_iota(jnp.int32, (experts, toks), 0) + first).astype(jnp.float32)

    def number(s, _):
        hit = jnp.zeros((experts, toks), jnp.float32)
        gate = jnp.zeros((experts, toks), jnp.float32)
        for j in range(top_k):
            same = route_ref[s, j:j + 1, :] == expert_row
            hit = jnp.where(same, 1.0, hit)
            gate = jnp.where(same, route_ref[s, top_k + j:top_k + j + 1, :], gate)
        lanes = [hit[:, lo:lo + 128] for lo in range(0, toks, 128)]
        inner = jnp.dot(jnp.concatenate(lanes, axis=0).astype(jnp.bfloat16), tri, preferred_element_type=jnp.float32)
        base = jnp.zeros((experts, 1), jnp.float32)
        parts = []
        for i in range(len(lanes)):
            if i * 128 % BLOCK == 0:
                for e in range(experts):
                    base_ref[s, i * 128 // BLOCK, e] = base[e, 0].astype(jnp.int32)
            part = inner[i * experts:(i + 1) * experts, :]
            parts.append(part + base)
            base = base + part[:, 127:128] + lanes[i][:, 127:128]
        for e in range(experts):
            base_ref[s, blocks, e] = base[e, 0].astype(jnp.int32)
        slot = jnp.concatenate(parts, axis=1)
        slot = jnp.where((hit > 0) & (slot < cap), slot, -1.0)
        slot_lane[s] = slot
        gate_lane[s] = gate
        slot_sub[s] = jnp.transpose(slot)
        return 0

    lax.fori_loop(0, sources, number, 0)

    def clear(i, _):
        where = pl.ds(pl.multiple_of(lax.rem(i, experts) * stride, 16), stride)
        rows_ref[i // experts, where, :] = jnp.zeros((stride, d_model), jnp.bfloat16)
        row_gate[i // experts, where, :] = jnp.zeros((stride, 1), jnp.float32)
        return 0

    lax.fori_loop(0, sources * experts, clear, 0)
    for copy in tok_copies:
        copy.wait()
    for copy in weight_copies(0, 0):
        copy.start()
    if adds:
        add_ref, sum_ref, add_sem = sum_refs
        add_copies = [pltpu.make_async_copy(add_hbm[i], add_ref.at[i], add_sem.at[i]) for i in range(adds)]
        for copy in add_copies:
            copy.start()

    def bounds(s, b, e):
        begin = jnp.minimum(base_ref[s, b, e], cap)
        end = jnp.minimum(base_ref[s, b + 1, e], cap)
        return begin, end, (begin // 16) * 16

    def extra_windows(s, b):
        most = jnp.int32(0)
        for e in range(experts):
            _, end, at = bounds(s, b, e)
            most = jnp.maximum(most, end - at)
        return jnp.maximum(most - 1, 0) // WINDOW

    def put_rows(s, e, at, begin, new, gates):
        head = pl.ds(pl.multiple_of(e * stride + at, 16), 16)
        rest = pl.ds(pl.multiple_of(e * stride + at + 16, 16), WINDOW - 16)
        old = lax.broadcasted_iota(jnp.int32, (16, 1), 0) + at < begin
        rows_ref[s, head, :] = jnp.where(old, rows_ref[s, head, :].astype(jnp.float32), new[:16]).astype(jnp.bfloat16)
        row_gate[s, head, :] = jnp.where(old, row_gate[s, head, :], gates[:16])
        rows_ref[s, rest, :] = new[16:].astype(jnp.bfloat16)
        row_gate[s, rest, :] = gates[16:]

    def dispatch(i, _):
        s, b = i // blocks, lax.rem(i, blocks)
        span = pl.ds(pl.multiple_of(b * BLOCK, BLOCK), BLOCK)
        local = lax.broadcasted_iota(jnp.int32, (WINDOW, BLOCK), 0)

        def one_hot(e, at):
            return (local + at).astype(jnp.float32) == slot_lane[s, e:e + 1, span]

        def gates_of(pick, e):
            return jnp.sum(jnp.where(pick, gate_lane[s, e:e + 1, span], 0.0), axis=1, keepdims=True)

        gates = []
        for e in range(experts):
            _, _, at = bounds(s, b, e)
            pick = one_hot(e, at)
            gates.append(gates_of(pick, e))
            pick_ref[e * WINDOW:(e + 1) * WINDOW, :] = pick.astype(jnp.bfloat16)
        new = jnp.dot(pick_ref[...], tok_ref[s, span, :], preferred_element_type=jnp.float32)
        for e in range(experts):
            begin, _, at = bounds(s, b, e)
            put_rows(s, e, at, begin, new[e * WINDOW:(e + 1) * WINDOW, :], gates[e])

        def more(j, _):
            k, e = j // experts + 1, lax.rem(j, experts)
            begin, _, at = bounds(s, b, e)
            at = at + k * WINDOW

            @pl.when(at < jnp.minimum(base_ref[s, b + 1, e], cap))
            def _():
                pick = (local + at).astype(jnp.float32) == slot_lane[s, pl.ds(e, 1), span]
                got = jnp.sum(jnp.where(pick, gate_lane[s, pl.ds(e, 1), span], 0.0), axis=1, keepdims=True)
                new = jnp.dot(pick.astype(jnp.bfloat16), tok_ref[s, span, :], preferred_element_type=jnp.float32)
                put_rows(s, e, at, begin, new, got)

            return 0

        lax.fori_loop(0, extra_windows(s, b) * experts, more, 0)
        return 0

    lax.fori_loop(0, sources * blocks, dispatch, 0)

    def tile(e, s, buf, lo, rows):
        where = pl.ds(pl.multiple_of(e * stride + lo, 16), rows)
        x = rows_ref[s, where, :]
        for at, width in chunks_of(main, CHUNK):
            a = jnp.dot(x, wg_buf[buf, :, at:at + width], preferred_element_type=jnp.float32)
            b = jnp.dot(x, wu_buf[buf, :, at:at + width], preferred_element_type=jnp.float32)
            h_ref[:rows, at:at + width] = (a * jax.nn.sigmoid(a) * b).astype(jnp.bfloat16)
        if main < ff:
            ab = jnp.dot(x, wx_buf[buf], preferred_element_type=jnp.float32)
            a, b = ab[:, :ff - main], ab[:, ff - main:]
            h_ref[:rows, main:] = (a * jax.nn.sigmoid(a) * b).astype(jnp.bfloat16)
        y = jnp.dot(h_ref[:rows, :], wd_buf[buf], preferred_element_type=jnp.float32)
        rows_ref[s, where, :] = (y * row_gate[s, where, :]).astype(jnp.bfloat16)

    def expert_step(e, _):
        buf = lax.rem(e, 2)
        for copy in weight_copies(e, buf):
            copy.wait()

        @pl.when(e + 1 < experts)
        def _():
            for copy in weight_copies(e + 1, 1 - buf):
                copy.start()

        def source_step(s, _):
            n = jnp.minimum(base_ref[s, blocks, e], cap)

            @pl.when(n > 0)
            def _():
                tile(e, s, buf, 0, small)

            if cap > small:

                @pl.when(n > small)
                def _():
                    tile(e, s, buf, small, cap - small)
            return 0

        lax.fori_loop(0, sources, source_step, 0)
        return 0

    lax.fori_loop(0, experts, expert_step, 0)

    def gather_rows(i, y_ref):
        s, b = i // blocks, lax.rem(i, blocks)
        span = pl.ds(pl.multiple_of(b * BLOCK, BLOCK), BLOCK)
        local = lax.broadcasted_iota(jnp.int32, (BLOCK, WINDOW), 1)
        puts = []
        for e in range(experts):
            _, _, at = bounds(s, b, e)
            puts.append(((local + at).astype(jnp.float32) == slot_sub[s, span, e:e + 1]).astype(jnp.bfloat16))
            y_ref[e * WINDOW:(e + 1) * WINDOW, :] = rows_ref[s, pl.ds(pl.multiple_of(e * stride + at, 16), WINDOW), :]
        return jnp.concatenate(puts, axis=1)

    def combine(half, put, y_ref):
        acc_ref[half] = jnp.dot(put, y_ref[...], preferred_element_type=jnp.float32)

    def finish(half, j):
        i = 2 * j + half
        s, b = i // blocks, lax.rem(i, blocks)
        span = pl.ds(pl.multiple_of(b * BLOCK, BLOCK), BLOCK)

        def more(j, _):
            k, e = j // experts + 1, lax.rem(j, experts)
            _, end, at = bounds(s, b, e)
            at = at + k * WINDOW

            @pl.when(at < end)
            def _():
                col = lax.broadcasted_iota(jnp.int32, (BLOCK, experts), 1)
                mine = jnp.sum(jnp.where(col == e, slot_sub[s, span, :], 0.0), axis=1, keepdims=True)
                slots = (lax.broadcasted_iota(jnp.int32, (BLOCK, WINDOW), 1) + at).astype(jnp.float32)
                y = rows_ref[s, pl.ds(pl.multiple_of(e * stride + at, 16), WINDOW), :]
                acc_ref[half] += jnp.dot((slots == mine).astype(jnp.bfloat16), y, preferred_element_type=jnp.float32)

            return 0

        lax.fori_loop(0, extra_windows(s, b) * experts, more, 0)

        if adds:

            @pl.when(s == 0)
            def _():
                total = acc_ref[half]
                for k in range(adds):
                    total += add_ref[k, span, :].astype(jnp.float32)
                sum_ref[span, :] = total
                pltpu.make_async_copy(sum_ref.at[span, :], out_hbm[0].at[span, :], out_sem).start()

        tok_ref[s, span, :] = acc_ref[half].astype(jnp.bfloat16)
        for t in range(1 if adds else 0, sources):

            @pl.when(s == t)
            def _():
                pltpu.make_async_copy(tok_ref.at[t, span, :], out_hbm[t].at[span, :], out_sem).start()
        return j

    if adds:
        for copy in add_copies:
            copy.wait()

    def pair(j, _):
        put_a = gather_rows(2 * j, yblk_ref)
        put_b = gather_rows(2 * j + 1, yblk2_ref)
        combine(0, put_a, yblk_ref)
        combine(1, put_b, yblk2_ref)
        lax.fori_loop(0, 2, finish, j)
        return 0

    lax.fori_loop(0, sources * blocks // 2, pair, 0)
    for s in range(sources):
        src = sum_ref if adds and s == 0 else tok_ref.at[s]
        pltpu.make_async_copy(src, out_hbm[s], out_sem).wait()


def phase(routes, toks, wg, wu, wd, cap, first=0, experts=None, adds=(), after=()):
    sources, _, tok_dev = routes.shape
    d_model = toks[0].shape[1]
    ff = wg.shape[2]
    main = ff // 256 * 256
    experts = experts or wg.shape[0]
    small = min(cap, 256)
    vm = pl.BlockSpec(memory_space=pltpu.VMEM)
    hbm = pl.BlockSpec(memory_space=pl.ANY)
    blocks = tok_dev // BLOCK
    height = experts * (cap + WINDOW)
    sum_scratch = [
        pltpu.VMEM((len(adds), tok_dev, d_model), jnp.bfloat16),
        pltpu.VMEM((tok_dev, d_model), jnp.float32),
        pltpu.SemaphoreType.DMA((len(adds),)),
    ] if adds else []
    return pl.pallas_call(
        functools.partial(phase_kernel, cap, small, first, experts, len(toks), len(adds), len(after)),
        out_shape=[
            jax.ShapeDtypeStruct((tok_dev, d_model), jnp.float32 if adds and s == 0 else jnp.bfloat16) for s in range(sources)
        ],
        in_specs=[vm] + [hbm] * (len(toks) + 3 + len(adds) + len(after)),
        out_specs=[hbm] * sources,
        scratch_shapes=[
            pltpu.VMEM((2, d_model, main), jnp.bfloat16),
            pltpu.VMEM((2, d_model, main), jnp.bfloat16),
            pltpu.VMEM((2, d_model, 2 * max(ff - main, 128)), jnp.bfloat16),
            pltpu.VMEM((2, ff, d_model), jnp.bfloat16),
            pltpu.VMEM((sources, tok_dev, d_model), jnp.bfloat16),
            pltpu.VMEM((sources, height, d_model), jnp.bfloat16),
            pltpu.VMEM((experts * WINDOW, BLOCK), jnp.bfloat16),
            pltpu.VMEM((experts * WINDOW, d_model), jnp.bfloat16),
            pltpu.VMEM((experts * WINDOW, d_model), jnp.bfloat16),
            pltpu.VMEM((2, BLOCK, d_model), jnp.float32),
            pltpu.VMEM((sources, experts, tok_dev), jnp.float32),
            pltpu.VMEM((sources, experts, tok_dev), jnp.float32),
            pltpu.VMEM((sources, tok_dev, experts), jnp.float32),
            pltpu.VMEM((sources, height, 1), jnp.float32),
            pltpu.VMEM((small, ff), jnp.bfloat16),
            pltpu.SMEM((sources, blocks + 1, experts), jnp.int32),
            pltpu.SemaphoreType.DMA((2, 3 * PARTS + 2)),
            pltpu.SemaphoreType.DMA((len(toks),)),
            pltpu.SemaphoreType.DMA,
        ] + sum_scratch,
        compiler_params=pltpu.CompilerParams(vmem_limit_bytes=67_000_000),
        cost_estimate=pl.CostEstimate(
            flops=6 * sources * experts * small * d_model * ff,
            bytes_accessed=6 * experts * d_model * ff,
            transcendentals=0,
        ),
        name="moe_phase",
    )(routes, *toks, wg, wu, wd, *adds, *after)


def solution(mesh):
    ep_size = mesh.shape["ep"]
    tp_size = mesh.shape["tp"]
    row_spec = P(("dp", "ep", "tp"), None)
    axes = ("dp", "ep", "tp")
    ranks = [(d, y, t) for d in range(mesh.shape["dp"]) for y in range(ep_size) for t in range(tp_size)]

    def rank_of(d, y, t):
        return (d * ep_size + y) * tp_size + t

    def shift(arr, flip_ep, flip_tp):
        return lax.ppermute(arr, axes, [(rank_of(*r), rank_of(r[0], r[1] ^ flip_ep, r[2] ^ flip_tp)) for r in ranks])

    def local_layer(tokens, expert_ids, gates, w_gate, w_up, w_down):
        tok_dev, _ = tokens.shape
        top_k = expert_ids.shape[1]
        local_experts = w_gate.shape[0]
        capacity = 5 * top_k * tok_dev // (4 * local_experts * ep_size)
        first = (lax.axis_index("ep") * local_experts).astype(jnp.float32)
        routes = jnp.concatenate([expert_ids.T.astype(jnp.float32), gates.T], axis=0)

        def run(tok_list, route_list, after=(), **part):
            stacked = jnp.stack(route_list)
            lines = jnp.arange(2 * top_k)[None, :, None] < top_k
            stacked = jnp.where(lines, stacked - first, stacked)
            return phase(stacked, tok_list, w_gate, w_up, w_down, capacity, after=after, **part)

        t_p, r_p = shift(tokens, 0, 1), shift(routes, 0, 1)
        r_x, r_y, t_x, t_y = shift(routes, 0, 2), shift(routes, 1, 0), shift(tokens, 0, 2), shift(tokens, 1, 0)
        own, own_p = run([tokens, t_p], [routes, r_p], experts=local_experts // 2)
        p_back = shift(own_p, 0, 1)
        r_x, r_y, t_x, t_y, own = lax.optimization_barrier((r_x, r_y, t_x, t_y, own))
        r_xp, t_xp = shift(r_x, 0, 1), shift(t_x, 0, 1)
        r_yp, t_yp = shift(r_y, 0, 1), shift(t_y, 0, 1)
        r_d, t_d = shift(r_x, 1, 0), shift(t_x, 1, 0)
        x_a, x_b = run([t_x, t_xp], [r_x, r_xp], after=(own,))
        x_back = shift(x_a, 0, 2)
        xp_back = shift(x_b, 0, 3)
        r_d, t_d, _ = lax.optimization_barrier((r_d, t_d, x_a))
        r_dp, t_dp = shift(r_d, 0, 1), shift(t_d, 0, 1)
        y_a, y_b = run([t_y, t_yp], [r_y, r_yp], after=(x_a,))
        y_back = shift(y_a, 1, 0)
        yp_back = shift(y_b, 1, 1)
        d_a, d_b = run([t_d, t_dp], [r_d, r_dp], after=(y_a,))
        d_in = shift(d_b, 0, 1)
        d_sum = add_pair(d_a, d_in)
        d_back = shift(d_sum, 1, 2)
        rest, rest_p = run(
            [tokens, t_p],
            [routes, r_p],
            after=(d_sum,),
            first=local_experts // 2,
            experts=local_experts // 2,
            adds=(own, p_back, x_back, xp_back, y_back, yp_back),
        )
        rest_back = shift(rest_p, 0, 1)
        total = rest + rest_back.astype(jnp.float32) + d_back.astype(jnp.float32)
        return total.astype(jnp.bfloat16)

    return jax.shard_map(
        local_layer,
        mesh=mesh,
        in_specs=(row_spec, row_spec, row_spec, P("ep", None, "tp"), P("ep", None, "tp"), P("ep", "tp", None)),
        out_specs=row_spec,
        check_vma=False,
    )
```

```python
import functools
import jax
import jax.numpy as jnp
from jax import lax
from jax.experimental import pallas as pl
from jax.experimental.pallas import tpu as pltpu

from jax.sharding import PartitionSpec as P


def add_pair(a, b):
    return (a.astype(jnp.float32) + b.astype(jnp.float32)).astype(jnp.bfloat16)


CHUNK = 512
BLOCK = 256
PARTS = 3
GROUP = 8
WINDOW = 128


def chunks_of(width, step):
    return [(lo, min(step, width - lo)) for lo in range(0, width, step)]


def phase_kernel(cap, small, first, experts, sources, pieces, adds, waits, rank_ref, *refs):
    route_hbm, refs = refs[:sources], refs[sources:]
    tok_hbm, refs = refs[:pieces], refs[pieces:]
    wg_hbm, wu_hbm, wd_hbm = refs[:3]
    add_hbm = refs[3:3 + adds]
    refs = refs[3 + adds + waits:]
    out_hbm = refs[:sources]
    (wg_buf, wu_buf, wx_buf, wd_buf, tok_ref, rows_ref, pick_ref, yblk_ref, yblk2_ref, acc_ref, slot_lane, gate_lane, slot_sub, row_gate, h_ref,
     base_ref, sems, tok_sems, out_sem, route_ref, route_sems, *sum_refs) = refs[sources:]
    _, lines, toks = route_ref.shape
    d_model = tok_ref.shape[2]
    top_k = lines // 2
    ff = wg_hbm.shape[2]
    blocks = toks // BLOCK
    stride = cap + WINDOW
    group_size = min(GROUP, experts)
    main = wg_buf.shape[2]

    def weight_copies(e, buf):
        at = first + e
        pairs = []
        for lo, rows in chunks_of(d_model, d_model // PARTS):
            part = pl.ds(lo, rows)
            pairs.append((wg_hbm.at[at, part, :main], wg_buf.at[buf, part, :]))
            pairs.append((wu_hbm.at[at, part, :main], wu_buf.at[buf, part, :]))
        if main < ff:
            pairs.append((wg_hbm.at[at, :, main:], wx_buf.at[buf, :, :ff - main]))
            pairs.append((wu_hbm.at[at, :, main:], wx_buf.at[buf, :, ff - main:]))
        for lo, rows in chunks_of(ff, ff // PARTS):
            pairs.append((wd_hbm.at[at, pl.ds(lo, rows), :], wd_buf.at[buf, pl.ds(lo, rows), :]))
        return [pltpu.make_async_copy(src, dst, sems.at[buf, i]) for i, (src, dst) in enumerate(pairs)]

    size = sources * toks // pieces
    tok_copies = [
        pltpu.make_async_copy(tok_hbm[p], tok_ref.at[p * size // toks, pl.ds(p * size % toks, size), :], tok_sems.at[p])
        for p in range(pieces)
    ]
    route_copies = [pltpu.make_async_copy(route_hbm[s], route_ref.at[s], route_sems.at[s]) for s in range(sources)]
    for copy in route_copies + tok_copies:
        copy.start()

    tri = (lax.broadcasted_iota(jnp.int32, (128, 128), 0) < lax.broadcasted_iota(jnp.int32, (128, 128), 1)).astype(jnp.bfloat16)
    expert_row = (lax.broadcasted_iota(jnp.int32, (experts, toks), 0) + first + rank_ref[0]).astype(jnp.float32)

    def number(s, _):
        hit = jnp.zeros((experts, toks), jnp.float32)
        gate = jnp.zeros((experts, toks), jnp.float32)
        for j in range(top_k):
            same = route_ref[s, j:j + 1, :] == expert_row
            hit = jnp.where(same, 1.0, hit)
            gate = jnp.where(same, route_ref[s, top_k + j:top_k + j + 1, :], gate)
        lanes = [hit[:, lo:lo + 128] for lo in range(0, toks, 128)]
        inner = jnp.dot(jnp.concatenate(lanes, axis=0).astype(jnp.bfloat16), tri, preferred_element_type=jnp.float32)
        base = jnp.zeros((experts, 1), jnp.float32)
        parts = []
        for i in range(len(lanes)):
            if i * 128 % BLOCK == 0:
                for e in range(experts):
                    base_ref[s, i * 128 // BLOCK, e] = base[e, 0].astype(jnp.int32)
            part = inner[i * experts:(i + 1) * experts, :]
            parts.append(part + base)
            base = base + part[:, 127:128] + lanes[i][:, 127:128]
        for e in range(experts):
            base_ref[s, blocks, e] = base[e, 0].astype(jnp.int32)
        slot = jnp.concatenate(parts, axis=1)
        slot = jnp.where((hit > 0) & (slot < cap), slot, -1.0)
        slot_lane[s] = slot
        gate_lane[s] = gate
        slot_sub[s] = jnp.transpose(slot)
        return 0

    for copy in route_copies:
        copy.wait()
    lax.fori_loop(0, sources, number, 0)
    for copy in weight_copies(0, 0):
        copy.start()

    def clear(i, _):
        where = pl.ds(pl.multiple_of(lax.rem(i, experts) * stride, 16), stride)
        rows_ref[i // experts, where, :] = jnp.zeros((stride, d_model), jnp.bfloat16)
        row_gate[i // experts, where, :] = jnp.zeros((stride, 1), jnp.float32)
        return 0

    lax.fori_loop(0, sources * experts, clear, 0)
    for copy in tok_copies:
        copy.wait()
    if adds:
        add_ref, sum_ref, add_sem = sum_refs
        add_copies = [pltpu.make_async_copy(add_hbm[i], add_ref.at[i], add_sem.at[i]) for i in range(adds)]
        for copy in add_copies:
            copy.start()

    def bounds(s, b, e):
        begin = jnp.minimum(base_ref[s, b, e], cap)
        end = jnp.minimum(base_ref[s, b + 1, e], cap)
        return begin, end, (begin // 16) * 16

    def extra_windows(s, b):
        most = jnp.int32(0)
        for e in range(experts):
            _, end, at = bounds(s, b, e)
            most = jnp.maximum(most, end - at)
        return jnp.maximum(most - 1, 0) // WINDOW

    def put_rows(s, e, at, begin, new, gates):
        head = pl.ds(pl.multiple_of(e * stride + at, 16), 16)
        rest = pl.ds(pl.multiple_of(e * stride + at + 16, 16), WINDOW - 16)
        old = lax.broadcasted_iota(jnp.int32, (16, 1), 0) + at < begin
        rows_ref[s, head, :] = jnp.where(old, rows_ref[s, head, :].astype(jnp.float32), new[:16]).astype(jnp.bfloat16)
        row_gate[s, head, :] = jnp.where(old, row_gate[s, head, :], gates[:16])
        rows_ref[s, rest, :] = new[16:].astype(jnp.bfloat16)
        row_gate[s, rest, :] = gates[16:]

    def dispatch(i, _):
        s, b = i // blocks, lax.rem(i, blocks)
        span = pl.ds(pl.multiple_of(b * BLOCK, BLOCK), BLOCK)
        local = lax.broadcasted_iota(jnp.int32, (WINDOW, BLOCK), 0)

        def group(g):
            gates = []
            for i in range(group_size):
                e = g * group_size + i
                _, _, at = bounds(s, b, e)
                pick = (local + at).astype(jnp.float32) == slot_lane[s, e:e + 1, span]
                gates.append(jnp.sum(jnp.where(pick, gate_lane[s, e:e + 1, span], 0.0), axis=1, keepdims=True))
                pick_ref[i * WINDOW:(i + 1) * WINDOW, :] = pick.astype(jnp.bfloat16)
            new = jnp.dot(pick_ref[...], tok_ref[s, span, :], preferred_element_type=jnp.float32)
            for i in range(group_size):
                e = g * group_size + i
                begin, _, at = bounds(s, b, e)
                put_rows(s, e, at, begin, new[i * WINDOW:(i + 1) * WINDOW, :], gates[i])

        for g in range(experts // group_size):
            group(g)

        def more(j, _):
            k, e = j // experts + 1, lax.rem(j, experts)
            begin, _, at = bounds(s, b, e)
            at = at + k * WINDOW

            @pl.when(at < jnp.minimum(base_ref[s, b + 1, e], cap))
            def _():
                pick = (local + at).astype(jnp.float32) == slot_lane[s, pl.ds(e, 1), span]
                got = jnp.sum(jnp.where(pick, gate_lane[s, pl.ds(e, 1), span], 0.0), axis=1, keepdims=True)
                new = jnp.dot(pick.astype(jnp.bfloat16), tok_ref[s, span, :], preferred_element_type=jnp.float32)
                put_rows(s, e, at, begin, new, got)

            return 0

        lax.fori_loop(0, extra_windows(s, b) * experts, more, 0)
        return 0

    lax.fori_loop(0, sources * blocks, dispatch, 0)

    def tile(e, s, buf, lo, rows):
        where = pl.ds(pl.multiple_of(e * stride + lo, 16), rows)
        x = rows_ref[s, where, :]
        for at, width in chunks_of(main, CHUNK):
            a = jnp.dot(x, wg_buf[buf, :, at:at + width], preferred_element_type=jnp.float32)
            b = jnp.dot(x, wu_buf[buf, :, at:at + width], preferred_element_type=jnp.float32)
            h_ref[:rows, at:at + width] = (a * jax.nn.sigmoid(a) * b).astype(jnp.bfloat16)
        if main < ff:
            ab = jnp.dot(x, wx_buf[buf], preferred_element_type=jnp.float32)
            a, b = ab[:, :ff - main], ab[:, ff - main:]
            h_ref[:rows, main:] = (a * jax.nn.sigmoid(a) * b).astype(jnp.bfloat16)
        y = jnp.dot(h_ref[:rows, :], wd_buf[buf], preferred_element_type=jnp.float32)
        rows_ref[s, where, :] = (y * row_gate[s, where, :]).astype(jnp.bfloat16)

    def expert_step(e, _):
        buf = lax.rem(e, 2)
        for copy in weight_copies(e, buf):
            copy.wait()

        @pl.when(e + 1 < experts)
        def _():
            for copy in weight_copies(e + 1, 1 - buf):
                copy.start()

        def source_step(s, _):
            n = jnp.minimum(base_ref[s, blocks, e], cap)

            @pl.when(n > 0)
            def _():
                tile(e, s, buf, 0, small)

            if cap > small:

                @pl.when(n > small)
                def _():
                    tile(e, s, buf, small, cap - small)
            return 0

        lax.fori_loop(0, sources, source_step, 0)
        return 0

    lax.fori_loop(0, experts, expert_step, 0)

    def gather_rows(i, y_ref):
        s, b = i // blocks, lax.rem(i, blocks)
        span = pl.ds(pl.multiple_of(b * BLOCK, BLOCK), BLOCK)
        local = lax.broadcasted_iota(jnp.int32, (BLOCK, WINDOW), 1)
        puts = []
        for e in range(experts):
            _, _, at = bounds(s, b, e)
            puts.append(((local + at).astype(jnp.float32) == slot_sub[s, span, e:e + 1]).astype(jnp.bfloat16))
            y_ref[e * WINDOW:(e + 1) * WINDOW, :] = rows_ref[s, pl.ds(pl.multiple_of(e * stride + at, 16), WINDOW), :]
        return jnp.concatenate(puts, axis=1)

    def combine(half, put, y_ref):
        acc_ref[half] = jnp.dot(put, y_ref[...], preferred_element_type=jnp.float32)

    def finish(half, j):
        i = 2 * j + half
        s, b = i // blocks, lax.rem(i, blocks)
        span = pl.ds(pl.multiple_of(b * BLOCK, BLOCK), BLOCK)

        def more(j, _):
            k, e = j // experts + 1, lax.rem(j, experts)
            _, end, at = bounds(s, b, e)
            at = at + k * WINDOW

            @pl.when(at < end)
            def _():
                col = lax.broadcasted_iota(jnp.int32, (BLOCK, experts), 1)
                mine = jnp.sum(jnp.where(col == e, slot_sub[s, span, :], 0.0), axis=1, keepdims=True)
                slots = (lax.broadcasted_iota(jnp.int32, (BLOCK, WINDOW), 1) + at).astype(jnp.float32)
                y = rows_ref[s, pl.ds(pl.multiple_of(e * stride + at, 16), WINDOW), :]
                acc_ref[half] += jnp.dot((slots == mine).astype(jnp.bfloat16), y, preferred_element_type=jnp.float32)

            return 0

        lax.fori_loop(0, extra_windows(s, b) * experts, more, 0)

        if adds:

            @pl.when(s == 0)
            def _():
                total = acc_ref[half]
                for k in range(adds):
                    total += add_ref[k, span, :].astype(jnp.float32)
                sum_ref[span, :] = total
                pltpu.make_async_copy(sum_ref.at[span, :], out_hbm[0].at[span, :], out_sem).start()

        tok_ref[s, span, :] = acc_ref[half].astype(jnp.bfloat16)
        for t in range(1 if adds else 0, sources):

            @pl.when(s == t)
            def _():
                pltpu.make_async_copy(tok_ref.at[t, span, :], out_hbm[t].at[span, :], out_sem).start()
        return j

    if adds:
        for copy in add_copies:
            copy.wait()

    def pair(j, _):
        put_a = gather_rows(2 * j, yblk_ref)
        put_b = gather_rows(2 * j + 1, yblk2_ref)
        combine(0, put_a, yblk_ref)
        combine(1, put_b, yblk2_ref)
        lax.fori_loop(0, 2, finish, j)
        return 0

    lax.fori_loop(0, sources * blocks // 2, pair, 0)
    for s in range(sources):
        src = sum_ref if adds and s == 0 else tok_ref.at[s]
        pltpu.make_async_copy(src, out_hbm[s], out_sem).wait()


def phase(rank, routes, toks, wg, wu, wd, cap, first=0, experts=None, adds=(), after=()):
    sources, (lines, tok_dev) = len(routes), routes[0].shape
    d_model = toks[0].shape[1]
    ff = wg.shape[2]
    main = ff // 256 * 256
    experts = experts or wg.shape[0]
    small = min(cap, 256)
    hbm = pl.BlockSpec(memory_space=pl.ANY)
    blocks = tok_dev // BLOCK
    height = experts * (cap + WINDOW)
    sum_scratch = [
        pltpu.VMEM((len(adds), tok_dev, d_model), jnp.bfloat16),
        pltpu.VMEM((tok_dev, d_model), jnp.float32),
        pltpu.SemaphoreType.DMA((len(adds),)),
    ] if adds else []
    return pl.pallas_call(
        functools.partial(phase_kernel, cap, small, first, experts, sources, len(toks), len(adds), len(after)),
        out_shape=[
            jax.ShapeDtypeStruct((tok_dev, d_model), jnp.float32 if adds and s == 0 else jnp.bfloat16) for s in range(sources)
        ],
        in_specs=[pl.BlockSpec(memory_space=pltpu.SMEM)] + [hbm] * (sources + len(toks) + 3 + len(adds) + len(after)),
        out_specs=[hbm] * sources,
        scratch_shapes=[
            pltpu.VMEM((2, d_model, main), jnp.bfloat16),
            pltpu.VMEM((2, d_model, main), jnp.bfloat16),
            pltpu.VMEM((2, d_model, 2 * max(ff - main, 128)), jnp.bfloat16),
            pltpu.VMEM((2, ff, d_model), jnp.bfloat16),
            pltpu.VMEM((sources, tok_dev, d_model), jnp.bfloat16),
            pltpu.VMEM((sources, height, d_model), jnp.bfloat16),
            pltpu.VMEM((min(GROUP, experts) * WINDOW, BLOCK), jnp.bfloat16),
            pltpu.VMEM((experts * WINDOW, d_model), jnp.bfloat16),
            pltpu.VMEM((experts * WINDOW, d_model), jnp.bfloat16),
            pltpu.VMEM((2, BLOCK, d_model), jnp.float32),
            pltpu.VMEM((sources, experts, tok_dev), jnp.float32),
            pltpu.VMEM((sources, experts, tok_dev), jnp.float32),
            pltpu.VMEM((sources, tok_dev, experts), jnp.float32),
            pltpu.VMEM((sources, height, 1), jnp.float32),
            pltpu.VMEM((small, ff), jnp.bfloat16),
            pltpu.SMEM((sources, blocks + 1, experts), jnp.int32),
            pltpu.SemaphoreType.DMA((2, 3 * PARTS + 2)),
            pltpu.SemaphoreType.DMA((len(toks),)),
            pltpu.SemaphoreType.DMA,
            pltpu.VMEM((sources, lines, tok_dev), jnp.float32),
            pltpu.SemaphoreType.DMA((sources,)),
        ] + sum_scratch,
        compiler_params=pltpu.CompilerParams(vmem_limit_bytes=67_000_000),
        cost_estimate=pl.CostEstimate(
            flops=6 * sources * experts * small * d_model * ff,
            bytes_accessed=6 * experts * d_model * ff,
            transcendentals=0,
        ),
        name="moe_phase",
    )(rank, *routes, *toks, wg, wu, wd, *adds, *after)


def solution(mesh):
    ep_size = mesh.shape["ep"]
    tp_size = mesh.shape["tp"]
    row_spec = P(("dp", "ep", "tp"), None)
    axes = ("dp", "ep", "tp")
    ranks = [(d, y, t) for d in range(mesh.shape["dp"]) for y in range(ep_size) for t in range(tp_size)]

    def rank_of(d, y, t):
        return (d * ep_size + y) * tp_size + t

    def shift(arr, flip_ep, flip_tp):
        return lax.ppermute(arr, axes, [(rank_of(*r), rank_of(r[0], r[1] ^ flip_ep, r[2] ^ flip_tp)) for r in ranks])

    def local_layer(tokens, expert_ids, gates, w_gate, w_up, w_down):
        tok_dev, _ = tokens.shape
        top_k = expert_ids.shape[1]
        local_experts = w_gate.shape[0]
        capacity = 5 * top_k * tok_dev // (4 * local_experts * ep_size)
        rank = (lax.axis_index("ep") * local_experts).astype(jnp.int32).reshape(1)
        routes = jnp.concatenate([expert_ids.T.astype(jnp.float32), gates.T], axis=0)

        def run(tok_list, route_list, after=(), **part):
            return phase(rank, route_list, tok_list, w_gate, w_up, w_down, capacity, after=after, **part)

        t_p, r_p = shift(tokens, 0, 1), shift(routes, 0, 1)
        r_x, r_y, t_x, t_y = shift(routes, 0, 2), shift(routes, 1, 0), shift(tokens, 0, 2), shift(tokens, 1, 0)
        own, own_p = run([tokens, t_p], [routes, r_p], experts=local_experts // 2)
        p_back = shift(own_p, 0, 1)
        r_x, r_y, t_x, t_y, own = lax.optimization_barrier((r_x, r_y, t_x, t_y, own))
        r_xp, t_xp = shift(r_x, 0, 1), shift(t_x, 0, 1)
        r_yp, t_yp = shift(r_y, 0, 1), shift(t_y, 0, 1)
        r_d, t_d = shift(r_x, 1, 0), shift(t_x, 1, 0)
        x_a, x_b = run([t_x, t_xp], [r_x, r_xp], after=(own,))
        x_back = shift(x_a, 0, 2)
        xp_back = shift(x_b, 0, 3)
        r_d, t_d, _ = lax.optimization_barrier((r_d, t_d, x_a))
        r_dp, t_dp = shift(r_d, 0, 1), shift(t_d, 0, 1)
        y_a, y_b = run([t_y, t_yp], [r_y, r_yp], after=(x_a,))
        y_back = shift(y_a, 1, 0)
        yp_back = shift(y_b, 1, 1)
        d_a, d_b = run([t_d, t_dp], [r_d, r_dp], after=(y_a,))
        d_in = shift(d_b, 0, 1)
        d_sum = add_pair(d_a, d_in)
        d_back = shift(d_sum, 1, 2)
        rest, rest_p = run(
            [tokens, t_p],
            [routes, r_p],
            after=(d_sum,),
            first=local_experts // 2,
            experts=local_experts // 2,
            adds=(own, p_back, x_back, xp_back, y_back, yp_back),
        )
        rest_back = shift(rest_p, 0, 1)
        total = rest + rest_back.astype(jnp.float32) + d_back.astype(jnp.float32)
        return total.astype(jnp.bfloat16)

    return jax.shard_map(
        local_layer,
        mesh=mesh,
        in_specs=(row_spec, row_spec, row_spec, P("ep", None, "tp"), P("ep", None, "tp"), P("ep", "tp", None)),
        out_specs=row_spec,
        check_vma=False,
    )
```
